32 devices in a mesh: members: 2 (over y), stars: 16 (over z, x, core).
Axes of the slice: x: 2, y: 2, z: 4, core: 2. Of those that a mesh axis runs over, the one named last changes fastest.
Arguments:
- position: float32 [3, 8192], P(None, ('members', 'stars')), parts along dimension 1, may hold values from -8 to 8
- velocity: float32 [3, 8192], P(None, ('members', 'stars')), parts along dimension 1, may hold values from -2 to 2
- acceleration: float32 [3, 8192], P(None, ('members', 'stars')), parts along dimension 1, may hold values from -2 to 2
- old_jerk: float32 [3, 8192], P(None, ('members', 'stars')), parts along dimension 1, may hold values from -6 to 6
- masses: float32 [8192], P(('members', 'stars')), parts along dimension 0, may hold values from 4.8828126e-05 to 0.0012207031
- levels: int32 [8192], P(('members', 'stars')), parts along dimension 0, may hold values from 0 to 3
- active_count: int32 [32], P(('members', 'stars')), parts along dimension 0, may hold values from 0 to 32, as said below
- active_slot: int32 [1024], P(('members', 'stars')), parts along dimension 0, may hold values from 0 to 255, as said below
Outputs:
- corrected: float32 [4, 3, 1024], P(None, None, ('members', 'stars')), parts along dimension 2
- derivatives: float32 [2, 3, 1024], P(None, None, ('members', 'stars')), parts along dimension 2
The draws below stay inside these ranges and needn't reach their ends.
There are 2 independent parts, one for each index of `members`. The reference program is written for one: setup_inputs(seed, part) draws one part's arguments, and reference() takes and returns one part's arrays. A program takes and returns all parts, laid end to end along the dimension named above; each array names one. Nothing has to cross between parts.
Inputs may be any that keep to these rules, and one draw needn't show every extreme that they name: `active_count`: the entries sum to 256; some entry equals 32 and some equals 0. `active_slot`: the 32 entries of one group are distinct; only its first active_count entries are live.
All inputs are finite; a program needn't handle non-finite values.
Results may differ from the reference program's by a relative error of at most 0.00002.
Values sent between devices are 32-bit elements; how exact they have to be, the bound alone decides.
A program may use at most 64 MiB of HBM per device.

```python
import math
import jax
import jax.numpy as jnp
from jax import lax

RES_DEV = 256
CAP = 32
OWNERS = 16
STARS = 4096


def draw_position(key, part):
    key_radius = jax.random.fold_in(key, 11)
    key_direction = jax.random.fold_in(key, 12)
    radius_scale = 0.6
    fraction = jax.random.uniform(key_radius, (STARS,), jnp.float32, 0.001, 0.995)
    radius = radius_scale / jnp.sqrt(jnp.power(fraction, -2.0 / 3.0) - 1.0)
    heading = jax.random.normal(key_direction, (3, STARS), jnp.float32)
    length = jnp.sqrt(jnp.sum(heading * heading, axis=0))
    heading = heading / jnp.maximum(length, 0.001)[None, :]
    placed = jnp.clip(radius[None, :] * heading, -8.0, 8.0)
    return placed.astype(jnp.float32)


def draw_active_count(key, part):
    half = CAP // 2
    shuffle = jax.random.permutation(jax.random.fold_in(key, 21), OWNERS)
    shifts = jax.random.randint(jax.random.fold_in(key, 22), (OWNERS // 2,), 0, half + 1)
    shifts = shifts.at[0].set(half)
    values = jnp.concatenate([half + shifts, half - shifts]).astype(jnp.int32)
    return jnp.zeros((OWNERS,), jnp.int32).at[shuffle].set(values)


def draw_active_slot(key, part):
    group_keys = jax.random.split(jax.random.fold_in(key, 31), OWNERS)

    def one_group(group_key):
        return jax.random.permutation(group_key, RES_DEV)[:CAP]
    return jax.vmap(one_group)(group_keys).reshape(-1).astype(jnp.int32)


def touch_ends(drawn, stream_key, smallest, top_value):
    longest = drawn.shape.index(max(drawn.shape))
    spots = []
    for shift in (0, 1):
        where = [jax.random.randint(jax.random.fold_in(stream_key, axis), (), 0, length) for axis, length in enumerate(drawn.shape)]
        where[longest] = (where[longest] + shift) % drawn.shape[longest]
        spots.append(tuple(where))
    return drawn.at[spots[0]].set(smallest).at[spots[1]].set(top_value)


def block_scale(rng, shape, cuts, low, top_value):
    def one(dim, parts):
        heights = jax.random.uniform(jax.random.fold_in(jax.random.fold_in(rng, 6), dim), (parts,), jnp.float32, low / len(cuts), top_value / len(cuts))
        return jnp.repeat(jnp.exp(heights), shape[dim] // parts).reshape((-1,) + (1,) * (len(shape) - dim - 1))

    gain = one(*cuts[0])
    for cut in cuts[1:]:
        gain = gain * one(*cut)
    return gain


def noise(key, dims, deviation, bound, cuts=(), kind=jnp.bfloat16):
    loudness = block_scale(key, dims, cuts, -0.22, 0.18) if cuts else 1.0
    drawn = jax.random.normal(key, dims, jnp.float32) * deviation * loudness
    return jnp.minimum(jnp.maximum(drawn, -bound), bound).astype(kind)


def setup_inputs(seed: int = 0, part: int = 0) -> dict:
    streams_of = jax.random.split(jax.random.key(seed), 9)
    part_keys = jax.random.split(jax.random.fold_in(streams_of[8], part), 9)
    return {
        "position": draw_position(jax.random.fold_in(jax.random.fold_in(streams_of[8], part), 71), part),
        "velocity": noise(part_keys[1], (3, STARS), 0.3, 2.0, ((1, 16),), jnp.float32),
        "acceleration": noise(part_keys[2], (3, STARS), 0.3, 2.0, ((1, 16),), jnp.float32),
        "old_jerk": noise(part_keys[3], (3, STARS), 1.0, 6.0, ((1, 16),), jnp.float32),
        "masses": jnp.clip(jnp.exp(math.log(0.0012207031) - 3.218876 * jax.random.uniform(part_keys[4], (STARS,), jnp.float32) ** block_scale(part_keys[4], (STARS,), ((0, 16),), -0.2, 0.2)), 4.882812572759576e-05, 0.0012207031),
        "levels": touch_ends(jax.random.randint(part_keys[5], (STARS,), 0, 4), jax.random.fold_in(part_keys[5], 1), 0, 3).astype(jnp.int32),
        "active_count": draw_active_count(jax.random.fold_in(jax.random.fold_in(streams_of[8], part), 71), part),
        "active_slot": draw_active_slot(jax.random.fold_in(jax.random.fold_in(streams_of[8], part), 71), part),
    }


SOFTEN = 0.0025
STEP_BASE = 0.5

def pair_terms(targets, res_pos, res_vel, res_mass):
    separation = res_pos[:, None, :] - targets[0:3, :, None]
    relative = res_vel[:, None, :] - targets[3:6, :, None]
    squared = lax.optimization_barrier(jnp.sum(separation * separation, axis=0)) + SOFTEN
    inverse = lax.rsqrt(squared)
    inverse_sq = inverse * inverse
    weight = res_mass[None, :] * inverse * inverse_sq
    radial = 3.0 * lax.optimization_barrier(jnp.sum(separation * relative, axis=0)) * inverse_sq
    pull = lax.optimization_barrier(jnp.sum(weight[None] * separation, axis=2))
    jerk_sum = lax.optimization_barrier(jnp.sum(weight[None] * (relative - radial[None] * separation), axis=2))
    return jnp.concatenate([pull, jerk_sum], axis=0)

def forces(targets, res_pos, res_vel, res_mass, block_limit):
    row_total = targets.shape[1]
    block_rows = row_total if row_total <= block_limit else math.gcd(row_total, block_limit)
    block_count = row_total // block_rows
    target_tiles = targets.reshape(6, block_count, block_rows).transpose(1, 0, 2)

    def one_tile(tile_cols):
        return pair_terms(tile_cols, res_pos, res_vel, res_mass)
    result = lax.map(one_tile, target_tiles)
    return result.transpose(1, 0, 2).reshape(6, row_total)

def predict(position, velocity, acceleration, old_jerk, levels):
    interval = STEP_BASE * jnp.exp2(-levels.astype(jnp.float32))
    moved_pos = position + interval * (velocity + interval * (0.5 * acceleration + interval * old_jerk / 6.0))
    moved_vel = velocity + interval * (acceleration + 0.5 * interval * old_jerk)
    return (moved_pos, moved_vel)

def correct(start_pos, start_vel, start_acc, start_jerk, new_acc, new_jerk, interval, live):
    end_vel = start_vel + 0.5 * interval * (start_acc + new_acc) + interval * interval * (start_jerk - new_jerk) / 12.0
    end_pos = start_pos + 0.5 * interval * (start_vel + end_vel) + interval * interval * (start_acc - new_acc) / 12.0
    differ = start_acc - new_acc
    snap_term = 3.0 * differ + interval * (start_jerk + 2.0 * new_jerk)
    crackle_term = 2.0 * differ + interval * (start_jerk + new_jerk)
    corrected = jnp.where(live[None, None], jnp.stack([end_pos, end_vel, new_acc, new_jerk]), 0.0)
    derivatives = jnp.where(live[None, None], jnp.stack([snap_term, crackle_term]), 0.0)
    return (corrected, derivatives)

def reference(position, velocity, acceleration, old_jerk, masses, levels, active_count, active_slot):
    owners = active_count.shape[0]
    capacity = active_slot.shape[0] // owners
    resident = position.shape[1] // owners
    slot_total = owners * capacity
    active_total = slot_total // 2
    moved_pos, moved_vel = predict(position, velocity, acceleration, old_jerk, levels)
    live = (jnp.arange(capacity, dtype=jnp.int32)[None, :] < active_count[:, None]).reshape(-1)
    global_index = (jnp.arange(owners, dtype=jnp.int32)[:, None] * resident + active_slot.reshape(owners, capacity)).reshape(-1).astype(jnp.int32)
    order_key = jnp.where(live, 0, slot_total).astype(jnp.int32) + jnp.arange(slot_total, dtype=jnp.int32)
    order_index = jnp.argsort(order_key, stable=True)[:active_total].astype(jnp.int32)
    chosen = global_index[order_index]
    targets = jnp.concatenate([moved_pos[:, chosen], moved_vel[:, chosen]], axis=0)
    summed = forces(targets, moved_pos, moved_vel, masses, 32)
    spread_out = jnp.zeros((6, slot_total), jnp.float32).at[:, order_index].set(summed)
    interval = STEP_BASE * jnp.exp2(-levels[global_index].astype(jnp.float32))
    return correct(position[:, global_index], velocity[:, global_index], acceleration[:, global_index], old_jerk[:, global_index], spread_out[0:3], spread_out[3:6], interval, live)
```

```python
import jax
import jax.numpy as jnp
from jax import lax
from jax.experimental import pallas as pl
from jax.experimental.pallas import tpu as pltpu
from jax.sharding import PartitionSpec as P

SOFTEN = 0.0025
STEP_BASE = 0.5
LANES = 128
HIGHEST = lax.Precision.HIGHEST


def dot(a, b, contract):
    return lax.dot_general(
        a, b, ((contract[:1], contract[1:]), ((), ())),
        precision=HIGHEST, preferred_element_type=jnp.float32,
    )


def power_of_half(level):
    scale = jnp.full(level.shape, STEP_BASE, jnp.float32)
    for bit in range(5):
        scale = jnp.where((level >> bit) & 1 == 1, scale * 0.5 ** (1 << bit), scale)
    return scale


def each(first, last, body):
    def step(k, carry):
        body(k)
        return carry

    lax.fori_loop(first, last, step, 0)


def kernel(n, pos_h, vel_h, acc_h, jerk_h, mass_h, level_h, slot_h,
           out_ref, der_ref,
           data, mass, level, slot, buf, in_sem, ready, lead_sem, send_sem, pass_sem, recv_sem):
    me = lax.axis_index("stars")
    stars = pos_h.shape[1]
    cap = slot_h.shape[1]
    chips = n // 2
    chip = me // 2
    side = me % 2
    partner = {"stars": me + 1 - 2 * side}
    mesh = pl.DeviceIdType.MESH

    loads = [
        pltpu.make_async_copy(pos_h, data.at[0, pl.ds(0, 3)], in_sem.at[0]),
        pltpu.make_async_copy(vel_h, data.at[1, pl.ds(0, 3)], in_sem.at[1]),
        pltpu.make_async_copy(acc_h, data.at[2, pl.ds(0, 3)], in_sem.at[2]),
        pltpu.make_async_copy(jerk_h, data.at[3, pl.ds(0, 3)], in_sem.at[3]),
        pltpu.make_async_copy(mass_h, mass, in_sem.at[4]),
        pltpu.make_async_copy(level_h, level, in_sem.at[5]),
        pltpu.make_async_copy(slot_h, slot, in_sem.at[6]),
    ]
    for load in loads:
        load.start()
    barrier = pltpu.get_barrier_semaphore()

    def signal(semaphore, device):
        pl.semaphore_signal(
            semaphore, inc=1, device_id={"stars": device}, device_id_type=mesh
        )

    signal(barrier, me + 1 - 2 * side)
    each(chip + 1, chips, lambda p: signal(barrier, 2 * p + 1))

    @pl.when((side == 1) | (chip == 0))
    def _():
        each(chip + 1, chips, lambda p: signal(barrier, 2 * p))

    for load in loads:
        load.wait()

    pos = data[0, 0:3]
    vel = data[1, 0:3]
    acc = data[2, 0:3]
    jerk = data[3, 0:3]
    step = power_of_half(level[...])
    moved_pos = pos + step * (vel + step * (0.5 * acc + step * jerk / 6.0))
    moved_vel = vel + step * (acc + 0.5 * step * jerk)
    own = buf.at[chip, side]
    own[0:3] = moved_pos
    own[3:6] = moved_vel
    own[6:7] = mass[...]
    own[7:8] = step

    far = chips // 2

    def across(other, part, done=send_sem):
        return pltpu.make_async_remote_copy(
            src_ref=own, dst_ref=own,
            send_sem=done, recv_sem=recv_sem.at[chip, part],
            device_id={"stars": other}, device_id_type=mesh,
        )

    def down(other, part):
        block = buf.at[other, part]
        return pltpu.make_async_remote_copy(
            src_ref=block, dst_ref=block,
            send_sem=pass_sem, recv_sem=recv_sem.at[other, part],
            device_id=partner, device_id_type=mesh,
        )

    pl.semaphore_wait(barrier, jnp.where(side == 1, 2 * chip, chip + jnp.minimum(chip, 1)) + 1)

    @pl.when(chip >= far)
    def _():
        across(0, side, lead_sem).start()

    each(0, chip, lambda p: across(2 * p + 1, side).start())
    swap = across(me + 1 - 2 * side, side)
    swap.start()

    @pl.when(side == 1)
    def _():
        each(0, 2 * chip, lambda p: signal(ready.at[chip], p))

    pick = (
        lax.broadcasted_iota(jnp.int32, (stars, cap), 0) == slot[...]
    ).astype(jnp.float32)
    moved = dot(own[...], pick, (1, 0))
    start_pos = dot(pos, pick, (1, 0))
    start_vel = dot(vel, pick, (1, 0))
    start_acc = dot(acc, pick, (1, 0))
    start_jerk = dot(jerk, pick, (1, 0))
    spread = (
        lax.broadcasted_iota(jnp.int32, (8, 6 * LANES), 1) // LANES
        == lax.broadcasted_iota(jnp.int32, (8, 6 * LANES), 0)
    ).astype(jnp.float32)
    spread_targets = dot(moved, spread, (0, 0))
    target = [spread_targets[:, c * LANES:(c + 1) * LANES] for c in range(6)]

    def add_block(j, part, sums):
        sums = list(sums)
        for first in range(0, stars, LANES):
            row = [buf[j, part, c:c + 1, first:first + LANES] for c in range(7)]
            d = [row[c] - target[c] for c in range(3)]
            w = [row[c + 3] - target[c + 3] for c in range(3)]
            q = d[0] * d[0] + d[1] * d[1] + d[2] * d[2] + SOFTEN
            u = lax.rsqrt(q)
            u2 = u * u
            weight = row[6] * u * u2
            radial = (d[0] * w[0] + d[1] * w[1] + d[2] * w[2]) * (3.0 * u2)
            for c in range(3):
                sums[c] += weight * d[c]
                sums[c + 3] += weight * (w[c] - radial * d[c])
        return tuple(sums)

    def arrive(k, sums):
        other = jnp.where(k < chips - chip, chip + k, chips - 1 - k)
        for part in (1, 0):
            copy = down(other, part)
            copy.wait_recv()

            @pl.when((side == 1) & ((chip > 0) | (other < far)))
            def _():
                copy.start()

            sums = add_block(other, part, sums)
        return sums

    sums = add_block(chip, side, (jnp.zeros((cap, LANES), jnp.float32),) * 6)

    def up(p):
        pl.semaphore_wait(ready.at[p], 1)
        across(2 * p + 1, side).start()

    each(chip + 1, chips, up)
    down(chip, 1 - side).wait_recv()
    sums = add_block(chip, 1 - side, sums)
    for k in range(1, chips):
        sums = arrive(k, sums)

    rest = jnp.concatenate(sums, axis=1)
    parts = []
    for _ in range(3):
        parts.append(rest.astype(jnp.bfloat16))
        rest = rest - parts[-1].astype(jnp.float32)
    width = 18 * LANES
    part_of = lax.rem(lax.broadcasted_iota(jnp.int32, (16, width), 1) // LANES, 6)
    row_of = lax.broadcasted_iota(jnp.int32, (16, width), 0)
    collect = (part_of + 5 * (part_of // 3) == row_of).astype(jnp.float32).astype(jnp.bfloat16)
    totals = lax.dot_general(
        collect, jnp.concatenate(parts, axis=1), (((1,), (1,)), ((), ())),
        preferred_element_type=jnp.float32,
    )
    new_acc = totals[0:3]
    new_jerk = totals[8:11]
    h = moved[7:8]
    end_vel = (
        start_vel + 0.5 * h * (start_acc + new_acc) + h * h * (start_jerk - new_jerk) / 12.0
    )
    end_pos = (
        start_pos + 0.5 * h * (start_vel + end_vel) + h * h * (start_acc - new_acc) / 12.0
    )
    differ = start_acc - new_acc
    snap = 3.0 * differ + h * (start_jerk + 2.0 * new_jerk)
    crackle = 2.0 * differ + h * (start_jerk + new_jerk)
    for place, value in enumerate((end_pos, end_vel, new_acc, new_jerk)):
        out_ref[:, place, :] = value
    for place, value in enumerate((snap, crackle)):
        der_ref[:, place, :] = value

    sent = buf.at[:, 0]
    pltpu.make_async_copy(sent, sent, send_sem).wait()

    @pl.when(chip >= far)
    def _():
        across(0, side, lead_sem).wait_send()

    @pl.when((side == 1) & (chip > 0))
    def _():
        passed = buf.at[pl.ds(1, chips - 1)]
        pltpu.make_async_copy(passed, passed, pass_sem).wait()

    if far > 1:
        @pl.when(me == 1)
        def _():
            passed = buf.at[pl.ds(1, far - 1)]
            pltpu.make_async_copy(passed, passed, pass_sem).wait()


def write_out(count, corrected, derivatives, out_ref, der_ref):
    for source, target in ((corrected, out_ref), (derivatives, der_ref)):
        live = lax.broadcasted_iota(jnp.int32, source.shape, 2) < count[0]
        target[...] = jnp.where(live, source[...], 0.0)


def build(n):
    def shards(position, velocity, acceleration, old_jerk, masses, levels, active_count, active_slot):
        stars = position.shape[1]
        cap = active_slot.shape[0]
        corrected, derivatives = pl.pallas_call(
            lambda *refs: kernel(n, *refs),
            out_shape=(
                pltpu.VMEM((3, 4, cap), jnp.float32),
                pltpu.VMEM((3, 2, cap), jnp.float32),
            ),
            in_specs=[pl.BlockSpec(memory_space=pltpu.HBM)] * 7,
            out_specs=(pl.BlockSpec(memory_space=pltpu.VMEM),) * 2,
            scratch_shapes=[
                pltpu.VMEM((4, 8, stars), jnp.float32),
                pltpu.VMEM((1, stars), jnp.float32),
                pltpu.VMEM((1, stars), jnp.int32),
                pltpu.VMEM((1, cap), jnp.int32),
                pltpu.VMEM((n // 2, 2, 8, stars), jnp.float32),
                pltpu.SemaphoreType.DMA((7,)),
                pltpu.SemaphoreType.REGULAR((n // 2,)),
                pltpu.SemaphoreType.DMA,
                pltpu.SemaphoreType.DMA,
                pltpu.SemaphoreType.DMA,
                pltpu.SemaphoreType.DMA((n // 2, 2)),
            ],
            compiler_params=pltpu.CompilerParams(collective_id=0, has_side_effects=True),
        )(
            position, velocity, acceleration, old_jerk,
            masses[None, :], levels[None, :], active_slot[None, :],
        )
        corrected = pltpu.with_memory_space_constraint(corrected, pltpu.VMEM)
        derivatives = pltpu.with_memory_space_constraint(derivatives, pltpu.VMEM)
        corrected, derivatives = pl.pallas_call(
            write_out,
            out_shape=(
                jax.ShapeDtypeStruct((3, 4, cap), jnp.float32),
                jax.ShapeDtypeStruct((3, 2, cap), jnp.float32),
            ),
            in_specs=[
                pl.BlockSpec(memory_space=pltpu.SMEM),
                pl.BlockSpec(memory_space=pltpu.VMEM),
                pl.BlockSpec(memory_space=pltpu.VMEM),
            ],
            out_specs=(pl.BlockSpec(memory_space=pltpu.VMEM),) * 2,
        )(active_count, corrected, derivatives)
        return corrected.transpose(1, 0, 2), derivatives.transpose(1, 0, 2)

    return shards


def solution(mesh):
    split = P(("members", "stars"))
    wide = P(None, ("members", "stars"))
    deep = P(None, None, ("members", "stars"))
    return jax.shard_map(
        build(mesh.shape["stars"]),
        mesh=mesh,
        in_specs=(wide, wide, wide, wide, split, split, split, split),
        out_specs=(deep, deep),
        check_vma=False,
    )
```

```python
import jax
import jax.numpy as jnp
from jax import lax
from jax.experimental import pallas as pl
from jax.experimental.pallas import tpu as pltpu
from jax.sharding import PartitionSpec as P

SOFTEN = 0.0025
STEP_BASE = 0.5
LANES = 128
HIGHEST = lax.Precision.HIGHEST


def dot(a, b, contract):
    return lax.dot_general(
        a, b, ((contract[:1], contract[1:]), ((), ())),
        precision=HIGHEST, preferred_element_type=jnp.float32,
    )


def power_of_half(level):
    scale = jnp.full(level.shape, STEP_BASE, jnp.float32)
    for bit in range(5):
        scale = jnp.where((level >> bit) & 1 == 1, scale * 0.5 ** (1 << bit), scale)
    return scale


def each(first, last, body):
    def step(k, carry):
        body(k)
        return carry

    lax.fori_loop(first, last, step, 0)


def swap_pairs(k, chips):
    moved = jnp.where(k % 2 == 1, k + 1, k - 1)
    return jnp.where((k == 0) | (moved >= chips), k, moved)


def kernel(n, pos_h, vel_h, acc_h, jerk_h, mass_h, level_h, slot_h,
           out_ref, der_ref,
           data8, mass, level, slot, total, collect, buf,
           in_sem, ready, send_sem, pass_sem, recv_sem):
    data = tuple(data8.at[k, pl.ds(0, 3)] for k in range(4))
    me = lax.axis_index("stars")
    stars = pos_h.shape[1]
    cap = slot_h.shape[1]
    chips = n // 2
    chip = swap_pairs(me // 2, chips)
    side = me % 2
    partner = {"stars": me + 1 - 2 * side}
    mesh = pl.DeviceIdType.MESH

    def finish(semaphore, rows):
        same = total.at[pl.ds(0, rows)]
        pltpu.make_async_copy(same, same, semaphore).wait()

    slot_load = pltpu.make_async_copy(slot_h, slot, in_sem.at[1])
    loads = [
        pltpu.make_async_copy(source, target, in_sem.at[0])
        for source, target in zip(
            (pos_h, vel_h, acc_h, jerk_h, mass_h, level_h), (*data, mass, level)
        )
    ]
    for load in loads:
        load.start()
    slot_load.start()
    barrier = pltpu.get_barrier_semaphore()

    def device_of(k, part):
        return 2 * swap_pairs(k, chips) + part

    def signal(semaphore, device):
        pl.semaphore_signal(
            semaphore, inc=1, device_id={"stars": device}, device_id_type=mesh
        )

    signal(barrier, me + 1 - 2 * side)

    @pl.when((side == 1) | (chip == 0))
    def _():
        each(chip + 1, chips, lambda p: signal(barrier, device_of(p, 1)))
        each(chip + 1, chips, lambda p: signal(barrier, device_of(p, 0)))

    pl.semaphore_wait(barrier, chip + jnp.minimum(chip, 1) + 1)

    @pl.when(side == 1)
    def _():
        each(0, chip, lambda p: signal(ready, device_of(p, 1)))

    finish(in_sem.at[0], 14)

    pos, vel, acc, jerk = (ref[...] for ref in data)
    step = power_of_half(level[...])
    moved_pos = pos + step * (vel + step * (0.5 * acc + step * jerk / 6.0))
    moved_vel = vel + step * (acc + 0.5 * step * jerk)
    own = buf.at[chip, side]
    own[0:3] = moved_pos
    own[3:6] = moved_vel
    own[6:7] = mass[...]
    own[7:8] = step

    far = chips // 2

    def across(other):
        return pltpu.make_async_remote_copy(
            src_ref=own, dst_ref=own,
            send_sem=send_sem, recv_sem=recv_sem.at[chip],
            device_id={"stars": other}, device_id_type=mesh,
        )

    def down(other):
        block = buf.at[other]
        return pltpu.make_async_remote_copy(
            src_ref=block, dst_ref=block,
            send_sem=pass_sem, recv_sem=recv_sem.at[other],
            device_id=partner, device_id_type=mesh,
        )

    @pl.when(chip >= far)
    def _():
        across(0).start()

    each(0, chip, lambda p: across(device_of(p, 1)).start())
    swap = across(me + 1 - 2 * side)
    swap.start()

    slot_load.wait()
    pick = (
        lax.broadcasted_iota(jnp.int32, (stars, cap), 0) == slot[...]
    ).astype(jnp.float32)
    moved = dot(own[...], pick, (1, 0))
    start_pos = dot(pos, pick, (1, 0))
    start_vel = dot(vel, pick, (1, 0))
    start_acc = dot(acc, pick, (1, 0))
    start_jerk = dot(jerk, pick, (1, 0))
    part_of = lax.broadcasted_iota(jnp.int32, collect.shape, 1) // LANES
    row_of = lax.broadcasted_iota(jnp.int32, collect.shape, 0)
    collect[...] = (
        part_of + jnp.where(part_of < 3, 0, 5) == row_of
    ).astype(jnp.float32).astype(jnp.bfloat16)
    h = moved[7:8]
    half_step = 0.5 * h
    twelfth = h * h / 12.0
    vel_base = start_vel + half_step * start_acc + twelfth * start_jerk
    pos_base = start_pos + half_step * start_vel + twelfth * start_acc
    snap_base = 3.0 * start_acc + h * start_jerk
    crackle_base = 2.0 * start_acc + h * start_jerk
    spread = (
        lax.broadcasted_iota(jnp.int32, (8, 6 * LANES), 1) // LANES
        == lax.broadcasted_iota(jnp.int32, (8, 6 * LANES), 0)
    ).astype(jnp.float32)
    spread_targets = dot(moved, spread, (0, 0))
    target = [spread_targets[:, c * LANES:(c + 1) * LANES] for c in range(6)]

    def add_block(j, part, sums):
        sums = list(sums)
        for first in range(0, stars, LANES):
            row = [buf[j, part, c:c + 1, first:first + LANES] for c in range(7)]
            d = [row[c] - target[c] for c in range(3)]
            w = [row[c + 3] - target[c + 3] for c in range(3)]
            q = d[0] * d[0] + d[1] * d[1] + d[2] * d[2] + SOFTEN
            u = lax.rsqrt(q)
            u2 = u * u
            weight = row[6] * u * u2
            radial = (d[0] * w[0] + d[1] * w[1] + d[2] * w[2]) * (3.0 * u2)
            for c in range(3):
                sums[c] += weight * d[c]
                sums[c + 3] += weight * (w[c] - radial * d[c])
        return tuple(sums)

    def arrive(k, sums):
        other = jnp.where(k < chips - chip, chip + k, chips - 1 - k)
        copy = down(other)
        copy.wait_recv()

        @pl.when((side == 1) & ((chip > 0) | (other < far)))
        def _():
            copy.start()

        return add_block(other, 0, add_block(other, 1, sums))

    sums = add_block(chip, side, (jnp.zeros((cap, LANES), jnp.float32),) * 6)

    @pl.when(chip < chips - 1)
    def _():
        pl.semaphore_wait(ready, jnp.where(side == 1, chips - 1 - chip, 1))

        @pl.when(side == 1)
        def _():
            signal(ready, me - 1)

        each(chip + 1, chips, lambda p: across(device_of(p, 1)).start())

    swap.wait_recv()
    sums = add_block(chip, 1 - side, sums)
    for k in range(1, chips):
        sums = arrive(k, sums)

    rest = jnp.concatenate(sums, axis=1)
    totals = None
    for _ in range(3):
        part = rest.astype(jnp.bfloat16)
        rest = rest - part.astype(jnp.float32)
        share = lax.dot_general(
            collect[...], part, (((1,), (1,)), ((), ())), preferred_element_type=jnp.float32
        )
        totals = share if totals is None else totals + share
    new_acc = totals[0:3]
    new_jerk = totals[8:11]
    end_vel = vel_base + half_step * new_acc - twelfth * new_jerk
    end_pos = pos_base + half_step * end_vel - twelfth * new_acc
    snap = snap_base - 3.0 * new_acc + 2.0 * h * new_jerk
    crackle = crackle_base - 2.0 * new_acc + h * new_jerk
    for place, value in enumerate((end_pos, end_vel, new_acc, new_jerk)):
        out_ref[:, place, :] = value
    for place, value in enumerate((snap, crackle)):
        der_ref[:, place, :] = value

    @pl.when(chip < far)
    def _():
        finish(send_sem, 8 * chips)

    @pl.when(chip >= far)
    def _():
        finish(send_sem, 8 * chips + 8)

    @pl.when((side == 1) & (chip > 0))
    def _():
        finish(pass_sem, 16 * chips - 16)

    if far > 1:
        @pl.when(me == 1)
        def _():
            finish(pass_sem, 16 * far - 16)


def write_out(count, corrected, derivatives, out_ref, der_ref):
    for source, target in ((corrected, out_ref), (derivatives, der_ref)):
        live = lax.broadcasted_iota(jnp.int32, source.shape, 2) < count[0]
        target[...] = jnp.where(live, source[...], 0.0)


def build(n):
    def shards(position, velocity, acceleration, old_jerk, masses, levels, active_count, active_slot):
        stars = position.shape[1]
        cap = active_slot.shape[0]
        corrected, derivatives = pl.pallas_call(
            lambda *refs: kernel(n, *refs),
            out_shape=(
                pltpu.VMEM((3, 4, cap), jnp.float32),
                pltpu.VMEM((3, 2, cap), jnp.float32),
            ),
            in_specs=[pl.BlockSpec(memory_space=pltpu.HBM)] * 7,
            out_specs=(pl.BlockSpec(memory_space=pltpu.VMEM),) * 2,
            scratch_shapes=[
                pltpu.VMEM((4, 8, stars), jnp.float32),
                pltpu.VMEM((1, stars), jnp.float32),
                pltpu.VMEM((1, stars), jnp.int32),
                pltpu.VMEM((1, cap), jnp.int32),
                pltpu.VMEM((8 * n, 1, stars), jnp.float32),
                pltpu.VMEM((16, 6 * LANES), jnp.bfloat16),
                pltpu.VMEM((n // 2, 2, 8, stars), jnp.float32),
                pltpu.SemaphoreType.DMA((2,)),
                pltpu.SemaphoreType.REGULAR,
                pltpu.SemaphoreType.DMA,
                pltpu.SemaphoreType.DMA,
                pltpu.SemaphoreType.DMA((n // 2,)),
            ],
            compiler_params=pltpu.CompilerParams(collective_id=0, has_side_effects=True),
        )(
            position, velocity, acceleration, old_jerk,
            masses[None, :], levels[None, :], active_slot[None, :],
        )
        corrected = pltpu.with_memory_space_constraint(corrected, pltpu.VMEM)
        derivatives = pltpu.with_memory_space_constraint(derivatives, pltpu.VMEM)
        corrected, derivatives = pl.pallas_call(
            write_out,
            out_shape=(
                jax.ShapeDtypeStruct((3, 4, cap), jnp.float32),
                jax.ShapeDtypeStruct((3, 2, cap), jnp.float32),
            ),
            in_specs=[
                pl.BlockSpec(memory_space=pltpu.SMEM),
                pl.BlockSpec(memory_space=pltpu.VMEM),
                pl.BlockSpec(memory_space=pltpu.VMEM),
            ],
            out_specs=(pl.BlockSpec(memory_space=pltpu.VMEM),) * 2,
        )(active_count, corrected, derivatives)
        return corrected.transpose(1, 0, 2), derivatives.transpose(1, 0, 2)

    return shards


def solution(mesh):
    split = P(("members", "stars"))
    wide = P(None, ("members", "stars"))
    deep = P(None, None, ("members", "stars"))
    return jax.shard_map(
        build(mesh.shape["stars"]),
        mesh=mesh,
        in_specs=(wide, wide, wide, wide, split, split, split, split),
        out_specs=(deep, deep),
        check_vma=False,
    )
```

```python
import jax
import jax.numpy as jnp
from jax import lax
from jax.experimental import pallas as pl
from jax.experimental.pallas import tpu as pltpu
from jax.sharding import PartitionSpec as P

SOFTEN = 0.0025
STEP_BASE = 0.5
LANES = 128
HIGHEST = lax.Precision.HIGHEST


def dot(a, b, contract):
    return lax.dot_general(
        a, b, ((contract[:1], contract[1:]), ((), ())),
        precision=HIGHEST, preferred_element_type=jnp.float32,
    )


def power_of_half(level):
    scale = jnp.full(level.shape, STEP_BASE, jnp.float32)
    for bit in range(5):
        scale = jnp.where((level >> bit) & 1 == 1, scale * 0.5 ** (1 << bit), scale)
    return scale


def each(first, last, body):
    def step(k, carry):
        body(k)
        return carry

    lax.fori_loop(first, last, step, 0)


def swap_pairs(k, chips):
    moved = jnp.where(k % 2 == 1, k + 1, k - 1)
    return jnp.where((k == 0) | (moved >= chips), k, moved)


def predict(pos, vel, acc, jerk, level):
    step = power_of_half(level)
    moved_pos = pos + step * (vel + step * (0.5 * acc + step * jerk / 6.0))
    moved_vel = vel + step * (acc + 0.5 * step * jerk)
    return moved_pos, moved_vel, step


def kernel(n, pos_h, vel_h, acc_h, jerk_h, mass_h, level_h, slot_h,
           out_ref, der_ref,
           data8, mass, level, slot, total, collect, far_data, far_mass, far_level, buf,
           in_sem, raw_sem, ready, send_sem, pass_sem, recv_sem):
    data = tuple(data8.at[k, pl.ds(0, 3)] for k in range(4))
    far_data = tuple(far_data.at[k, pl.ds(0, 3)] for k in range(4)) + (far_mass, far_level)
    me = lax.axis_index("stars")
    stars = pos_h.shape[1]
    cap = slot_h.shape[1]
    chips = n // 2
    chip = swap_pairs(me // 2, chips)
    side = me % 2
    partner = {"stars": me + 1 - 2 * side}
    mesh = pl.DeviceIdType.MESH

    def finish(semaphore, rows):
        same = total.at[pl.ds(0, rows)]
        pltpu.make_async_copy(same, same, semaphore).wait()

    slot_load = pltpu.make_async_copy(slot_h, slot, in_sem.at[1])
    loads = [
        pltpu.make_async_copy(source, target, in_sem.at[0])
        for source, target in zip(
            (pos_h, vel_h, acc_h, jerk_h, mass_h, level_h), (*data, mass, level)
        )
    ]
    for load in loads:
        load.start()
    slot_load.start()
    barrier = pltpu.get_barrier_semaphore()

    def device_of(k, part):
        return 2 * swap_pairs(k, chips) + part

    def signal(semaphore, device):
        pl.semaphore_signal(
            semaphore, inc=1, device_id={"stars": device}, device_id_type=mesh
        )

    signal(barrier, me + 1 - 2 * side)

    @pl.when((side == 1) | (chip == 0))
    def _():
        each(chip + 1, chips, lambda p: signal(barrier, device_of(p, 1)))
        each(chip + 1, chips, lambda p: signal(barrier, device_of(p, 0)))

    pl.semaphore_wait(barrier, chip + jnp.minimum(chip, 1) + 1)

    last = (chip == chips - 1) & (side == 0)

    @pl.when(last)
    def _():
        for device in range(2):
            for source, target in zip(
                (pos_h, vel_h, acc_h, jerk_h, mass_h, level_h), far_data
            ):
                pltpu.make_async_remote_copy(
                    src_ref=source, dst_ref=target, send_sem=send_sem, recv_sem=raw_sem,
                    device_id={"stars": device}, device_id_type=mesh,
                ).start()

    @pl.when(side == 1)
    def _():
        each(0, chip, lambda p: signal(ready, device_of(p, 1)))

    finish(in_sem.at[0], 14)

    pos, vel, acc, jerk = (ref[...] for ref in data)
    moved_pos, moved_vel, step = predict(pos, vel, acc, jerk, level[...])
    own = buf.at[chip, side]
    own[0:3] = moved_pos
    own[3:6] = moved_vel
    own[6:7] = mass[...]
    own[7:8] = step

    far = chips // 2

    def across(other):
        return pltpu.make_async_remote_copy(
            src_ref=own, dst_ref=own,
            send_sem=send_sem, recv_sem=recv_sem.at[chip],
            device_id={"stars": other}, device_id_type=mesh,
        )

    def half(other, part):
        block = buf.at[other, part]
        return pltpu.make_async_remote_copy(
            src_ref=block, dst_ref=block, send_sem=send_sem, recv_sem=recv_sem.at[other],
            device_id=partner, device_id_type=mesh,
        )

    def down(other):
        block = buf.at[other]
        return pltpu.make_async_remote_copy(
            src_ref=block, dst_ref=block,
            send_sem=pass_sem, recv_sem=recv_sem.at[other],
            device_id=partner, device_id_type=mesh,
        )

    @pl.when((chip >= far) & ~last)
    def _():
        across(0).start()

    each(jnp.where(last, 1, 0), chip, lambda p: across(device_of(p, 1)).start())
    swap = across(me + 1 - 2 * side)
    swap.start()

    slot_load.wait()
    pick = (
        lax.broadcasted_iota(jnp.int32, (stars, cap), 0) == slot[...]
    ).astype(jnp.float32)
    moved = dot(own[...], pick, (1, 0))
    start_pos = dot(pos, pick, (1, 0))
    start_vel = dot(vel, pick, (1, 0))
    start_acc = dot(acc, pick, (1, 0))
    start_jerk = dot(jerk, pick, (1, 0))
    part_of = lax.broadcasted_iota(jnp.int32, collect.shape, 1) // LANES
    row_of = lax.broadcasted_iota(jnp.int32, collect.shape, 0)
    collect[...] = (
        part_of + jnp.where(part_of < 3, 0, 5) == row_of
    ).astype(jnp.float32).astype(jnp.bfloat16)
    h = moved[7:8]
    half_step = 0.5 * h
    twelfth = h * h / 12.0
    vel_base = start_vel + half_step * start_acc + twelfth * start_jerk
    pos_base = start_pos + half_step * start_vel + twelfth * start_acc
    snap_base = 3.0 * start_acc + h * start_jerk
    crackle_base = 2.0 * start_acc + h * start_jerk
    spread = (
        lax.broadcasted_iota(jnp.int32, (8, 6 * LANES), 1) // LANES
        == lax.broadcasted_iota(jnp.int32, (8, 6 * LANES), 0)
    ).astype(jnp.float32)
    spread_targets = dot(moved, spread, (0, 0))
    target = [spread_targets[:, c * LANES:(c + 1) * LANES] for c in range(6)]

    def add_block(j, part, sums):
        sums = list(sums)
        for first in range(0, stars, LANES):
            row = [buf[j, part, c:c + 1, first:first + LANES] for c in range(7)]
            d = [row[c] - target[c] for c in range(3)]
            w = [row[c + 3] - target[c + 3] for c in range(3)]
            q = d[0] * d[0] + d[1] * d[1] + d[2] * d[2] + SOFTEN
            u = lax.rsqrt(q)
            u2 = u * u
            weight = row[6] * u * u2
            radial = (d[0] * w[0] + d[1] * w[1] + d[2] * w[2]) * (3.0 * u2)
            for c in range(3):
                sums[c] += weight * d[c]
                sums[c + 3] += weight * (w[c] - radial * d[c])
        return tuple(sums)

    def arrive(k, sums):
        other = jnp.where(k < chips - chip, chip + k, chips - 1 - k)
        copy = down(other)
        if k < chips - 1:
            copy.wait_recv()
        else:
            @pl.when(chip > 0)
            def _():
                copy.wait_recv()

            @pl.when(chip == 0)
            def _():
                half(k, 1).wait_recv()
                block = buf.at[k, 0]
                finish(raw_sem, 14)
                block[0:3], block[3:6], _ = predict(
                    *(ref[...] for ref in far_data[:4]), far_data[5][...]
                )
                block[6:7] = far_data[4][...]

        @pl.when((side == 1) & ((chip > 0) | (other < far)))
        def _():
            copy.start()

        return add_block(other, 0, add_block(other, 1, sums))

    sums = add_block(chip, side, (jnp.zeros((cap, LANES), jnp.float32),) * 6)

    @pl.when(chip < chips - 1)
    def _():
        pl.semaphore_wait(ready, jnp.where(side == 1, chips - 1 - chip, 1))

        @pl.when(side == 1)
        def _():
            signal(ready, me - 1)

        each(chip + 1, chips, lambda p: across(device_of(p, 1)).start())

    swap.wait_recv()
    sums = add_block(chip, 1 - side, sums)
    for k in range(1, chips):
        sums = arrive(k, sums)

    rest = jnp.concatenate(sums, axis=1)
    totals = None
    for _ in range(3):
        part = rest.astype(jnp.bfloat16)
        rest = rest - part.astype(jnp.float32)
        share = lax.dot_general(
            collect[...], part, (((1,), (1,)), ((), ())), preferred_element_type=jnp.float32
        )
        totals = share if totals is None else totals + share
    new_acc = totals[0:3]
    new_jerk = totals[8:11]
    end_vel = vel_base + half_step * new_acc - twelfth * new_jerk
    end_pos = pos_base + half_step * end_vel - twelfth * new_acc
    snap = snap_base - 3.0 * new_acc + 2.0 * h * new_jerk
    crackle = crackle_base - 2.0 * new_acc + h * new_jerk
    for place, value in enumerate((end_pos, end_vel, new_acc, new_jerk)):
        out_ref[:, place, :] = value
    for place, value in enumerate((snap, crackle)):
        der_ref[:, place, :] = value

    @pl.when(chip < far)
    def _():
        finish(send_sem, 8 * chips)

    @pl.when((chip >= far) & ~last)
    def _():
        finish(send_sem, 8 * chips + 8)

    @pl.when(last)
    def _():
        finish(send_sem, 8 * chips + 20)

    @pl.when((side == 1) & (chip > 0))
    def _():
        finish(pass_sem, 16 * chips - 16)

    if far > 1:
        @pl.when(me == 1)
        def _():
            finish(pass_sem, 16 * far - 16)


def write_out(count, corrected, derivatives, out_ref, der_ref):
    for source, target in ((corrected, out_ref), (derivatives, der_ref)):
        live = lax.broadcasted_iota(jnp.int32, source.shape, 2) < count[0]
        target[...] = jnp.where(live, source[...], 0.0)


def build(n):
    def shards(position, velocity, acceleration, old_jerk, masses, levels, active_count, active_slot):
        stars = position.shape[1]
        cap = active_slot.shape[0]
        corrected, derivatives = pl.pallas_call(
            lambda *refs: kernel(n, *refs),
            out_shape=(
                pltpu.VMEM((3, 4, cap), jnp.float32),
                pltpu.VMEM((3, 2, cap), jnp.float32),
            ),
            in_specs=[pl.BlockSpec(memory_space=pltpu.HBM)] * 7,
            out_specs=(pl.BlockSpec(memory_space=pltpu.VMEM),) * 2,
            scratch_shapes=[
                pltpu.VMEM((4, 8, stars), jnp.float32),
                pltpu.VMEM((1, stars), jnp.float32),
                pltpu.VMEM((1, stars), jnp.int32),
                pltpu.VMEM((1, cap), jnp.int32),
                pltpu.VMEM((8 * n, 1, stars), jnp.float32),
                pltpu.VMEM((16, 6 * LANES), jnp.bfloat16),
                pltpu.VMEM((4, 8, stars), jnp.float32),
                pltpu.VMEM((1, stars), jnp.float32),
                pltpu.VMEM((1, stars), jnp.int32),
                pltpu.VMEM((n // 2, 2, 8, stars), jnp.float32),
                pltpu.SemaphoreType.DMA((2,)),
                pltpu.SemaphoreType.DMA,
                pltpu.SemaphoreType.REGULAR,
                pltpu.SemaphoreType.DMA,
                pltpu.SemaphoreType.DMA,
                pltpu.SemaphoreType.DMA((n // 2,)),
            ],
            compiler_params=pltpu.CompilerParams(collective_id=0, has_side_effects=True),
        )(
            position, velocity, acceleration, old_jerk,
            masses[None, :], levels[None, :], active_slot[None, :],
        )
        corrected = pltpu.with_memory_space_constraint(corrected, pltpu.VMEM)
        derivatives = pltpu.with_memory_space_constraint(derivatives, pltpu.VMEM)
        corrected, derivatives = pl.pallas_call(
            write_out,
            out_shape=(
                jax.ShapeDtypeStruct((3, 4, cap), jnp.float32),
                jax.ShapeDtypeStruct((3, 2, cap), jnp.float32),
            ),
            in_specs=[
                pl.BlockSpec(memory_space=pltpu.SMEM),
                pl.BlockSpec(memory_space=pltpu.VMEM),
                pl.BlockSpec(memory_space=pltpu.VMEM),
            ],
            out_specs=(pl.BlockSpec(memory_space=pltpu.VMEM),) * 2,
        )(active_count, corrected, derivatives)
        return corrected.transpose(1, 0, 2), derivatives.transpose(1, 0, 2)

    return shards


def solution(mesh):
    split = P(("members", "stars"))
    wide = P(None, ("members", "stars"))
    deep = P(None, None, ("members", "stars"))
    return jax.shard_map(
        build(mesh.shape["stars"]),
        mesh=mesh,
        in_specs=(wide, wide, wide, wide, split, split, split, split),
        out_specs=(deep, deep),
        check_vma=False,
    )
```

```python
import jax
import jax.numpy as jnp
from jax import lax
from jax.experimental import pallas as pl
from jax.experimental.pallas import tpu as pltpu
from jax.sharding import PartitionSpec as P

SOFTEN = 0.0025
STEP_BASE = 0.5
LANES = 128
HIGHEST = lax.Precision.HIGHEST


def dot(a, b, contract):
    return lax.dot_general(
        a, b, ((contract[:1], contract[1:]), ((), ())),
        precision=HIGHEST, preferred_element_type=jnp.float32,
    )


def power_of_half(level):
    scale = jnp.full(level.shape, STEP_BASE, jnp.float32)
    for bit in range(5):
        scale = jnp.where((level >> bit) & 1 == 1, scale * 0.5 ** (1 << bit), scale)
    return scale


def each(first, last, body):
    def step(k, carry):
        body(k)
        return carry

    lax.fori_loop(first, last, step, 0)


def predict(pos, vel, acc, jerk, level):
    step = power_of_half(level)
    moved_pos = pos + step * (vel + step * (0.5 * acc + step * jerk / 6.0))
    moved_vel = vel + step * (acc + 0.5 * step * jerk)
    return moved_pos, moved_vel, step


def kernel(n, pos_h, vel_h, acc_h, jerk_h, mass_h, level_h, slot_h,
           out_ref, der_ref,
           data8, mass, level, slot, total, collect, far_data, far_mass, far_level, buf,
           in_sem, raw_sem, mate, ready, send_sem, pass_sem, recv_sem):
    data = tuple(data8.at[k, pl.ds(0, 3)] for k in range(4))
    far_data = tuple(far_data.at[k, pl.ds(0, 3)] for k in range(4)) + (far_mass, far_level)
    me = lax.axis_index("stars")
    stars = pos_h.shape[1]
    cap = slot_h.shape[1]
    chips = n // 2
    chip = me // 2
    side = me % 2
    top = chips - 1
    below = jnp.where(chip == top, top, jnp.minimum(chip, 1))
    above = jnp.where(chip == 0, 1, jnp.where(chip == top, chips, top))
    partner = {"stars": me + 1 - 2 * side}
    mesh = pl.DeviceIdType.MESH

    def finish(semaphore, rows):
        same = total.at[pl.ds(0, rows)]
        pltpu.make_async_copy(same, same, semaphore).wait()

    slot_load = pltpu.make_async_copy(slot_h, slot, in_sem.at[1])
    loads = [
        pltpu.make_async_copy(source, target, in_sem.at[0])
        for source, target in zip(
            (pos_h, vel_h, acc_h, jerk_h, mass_h, level_h), (*data, mass, level)
        )
    ]
    for load in loads:
        load.start()
    slot_load.start()
    barrier = pltpu.get_barrier_semaphore()

    def signal(semaphore, device):
        pl.semaphore_signal(
            semaphore, inc=1, device_id={"stars": device}, device_id_type=mesh
        )

    @pl.when(side == 1)
    def _():
        signal(barrier, me - 1)

    @pl.when((side == 1) | (chip == 0))
    def _():
        each(above, chips, lambda p: signal(barrier, 2 * p + 1))
        each(above, chips, lambda p: signal(barrier, 2 * p))

    entered = below + jnp.minimum(chip, 1) + 1 - side

    @pl.when(entered > 0)
    def _():
        pl.semaphore_wait(barrier, entered)

    @pl.when(side == 0)
    def _():
        signal(mate, me + 1)

    last = (chip == top) & (side == 0)

    @pl.when(last)
    def _():
        for device in range(1):
            for source, target in zip(
                (pos_h, vel_h, acc_h, jerk_h, mass_h, level_h), far_data
            ):
                pltpu.make_async_remote_copy(
                    src_ref=source, dst_ref=target, send_sem=send_sem, recv_sem=raw_sem,
                    device_id={"stars": device}, device_id_type=mesh,
                ).start()

    @pl.when((chip == top) & (side == 1))
    def _():
        each(0, top, lambda p: signal(ready, 2 * p + 1))

    finish(in_sem.at[0], 14)

    pos, vel, acc, jerk = (ref[...] for ref in data)
    moved_pos, moved_vel, step = predict(pos, vel, acc, jerk, level[...])
    own = buf.at[chip, side]
    own[0:3] = moved_pos
    own[3:6] = moved_vel
    own[6:7] = mass[...]
    own[7:8] = step

    far = chips // 2

    def across(other):
        return pltpu.make_async_remote_copy(
            src_ref=own, dst_ref=own,
            send_sem=send_sem, recv_sem=recv_sem.at[chip],
            device_id={"stars": other}, device_id_type=mesh,
        )

    def half(other, part):
        block = buf.at[other, part]
        return pltpu.make_async_remote_copy(
            src_ref=block, dst_ref=block, send_sem=send_sem, recv_sem=recv_sem.at[other],
            device_id=partner, device_id_type=mesh,
        )

    def down(other):
        block = buf.at[other]
        return pltpu.make_async_remote_copy(
            src_ref=block, dst_ref=block,
            send_sem=pass_sem, recv_sem=recv_sem.at[other],
            device_id=partner, device_id_type=mesh,
        )

    @pl.when((chip >= far) & (side == 0) & ~last)
    def _():
        across(0).start()

    each(0, jnp.minimum(below, 1), lambda p: across(2 * p + 1).start())

    @pl.when((chip >= far) & (side == 1))
    def _():
        across(0).start()

    each(1, below, lambda p: across(2 * p + 1).start())
    swap = across(me + 1 - 2 * side)

    @pl.when(side == 1)
    def _():
        pl.semaphore_wait(mate, 1)

    swap.start()

    slot_load.wait()
    pick = (
        lax.broadcasted_iota(jnp.int32, (stars, cap), 0) == slot[...]
    ).astype(jnp.float32)
    moved = dot(own[...], pick, (1, 0))
    start_pos = dot(pos, pick, (1, 0))
    start_vel = dot(vel, pick, (1, 0))
    start_acc = dot(acc, pick, (1, 0))
    start_jerk = dot(jerk, pick, (1, 0))
    part_of = lax.broadcasted_iota(jnp.int32, collect.shape, 1) // LANES
    row_of = lax.broadcasted_iota(jnp.int32, collect.shape, 0)
    collect[...] = (
        part_of + jnp.where(part_of < 3, 0, 5) == row_of
    ).astype(jnp.float32).astype(jnp.bfloat16)
    h = moved[7:8]
    half_step = 0.5 * h
    twelfth = h * h / 12.0
    vel_base = start_vel + half_step * start_acc + twelfth * start_jerk
    pos_base = start_pos + half_step * start_vel + twelfth * start_acc
    snap_base = 3.0 * start_acc + h * start_jerk
    crackle_base = 2.0 * start_acc + h * start_jerk
    spread = (
        lax.broadcasted_iota(jnp.int32, (8, 6 * LANES), 1) // LANES
        == lax.broadcasted_iota(jnp.int32, (8, 6 * LANES), 0)
    ).astype(jnp.float32)
    spread_targets = dot(moved, spread, (0, 0))
    target = [spread_targets[:, c * LANES:(c + 1) * LANES] for c in range(6)]

    def add_block(j, part, sums):
        sums = list(sums)
        for first in range(0, stars, LANES):
            row = [buf[j, part, c:c + 1, first:first + LANES] for c in range(7)]
            d = [row[c] - target[c] for c in range(3)]
            w = [row[c + 3] - target[c + 3] for c in range(3)]
            q = d[0] * d[0] + d[1] * d[1] + d[2] * d[2] + SOFTEN
            u = lax.rsqrt(q)
            u2 = u * u
            weight = row[6] * u * u2
            radial = (d[0] * w[0] + d[1] * w[1] + d[2] * w[2]) * (3.0 * u2)
            for c in range(3):
                sums[c] += weight * d[c]
                sums[c + 3] += weight * (w[c] - radial * d[c])
        return tuple(sums)

    def arrive(k, sums):
        other = jnp.where(chip == 0, k, chips - k - jnp.where(chips - k > chip, 0, 1))
        copy = down(other)
        if k < chips - 1:
            copy.wait_recv()
        else:
            @pl.when(me > 0)
            def _():
                copy.wait_recv()

            @pl.when(me == 0)
            def _():
                half(k, 1).wait_recv()

        @pl.when((side == 1) & ((chip > 0) | (other < far)))
        def _():
            copy.start()

        sums = add_block(other, 1, sums)
        if k == chips - 1:
            @pl.when(me == 0)
            def _():
                finish(raw_sem, 14)
                block = buf.at[k, 0]
                block[0:3], block[3:6], _ = predict(
                    *(ref[...] for ref in far_data[:4]), far_data[5][...]
                )
                block[6:7] = far_data[4][...]

        return add_block(other, 0, sums)

    sums = add_block(chip, side, (jnp.zeros((cap, LANES), jnp.float32),) * 6)

    @pl.when(chip < top)
    def _():
        pl.semaphore_wait(ready, 1)

        @pl.when(side == 1)
        def _():
            signal(ready, me - 1)

        each(below, chip, lambda p: across(2 * p + 1).start())
        each(chip + 1, chips, lambda p: across(2 * p + 1).start())

    swap.wait_recv()
    sums = add_block(chip, 1 - side, sums)
    for k in range(1, chips):
        sums = arrive(k, sums)

    rest = jnp.concatenate(sums, axis=1)
    totals = None
    for _ in range(3):
        part = rest.astype(jnp.bfloat16)
        rest = rest - part.astype(jnp.float32)
        share = lax.dot_general(
            collect[...], part, (((1,), (1,)), ((), ())), preferred_element_type=jnp.float32
        )
        totals = share if totals is None else totals + share
    new_acc = totals[0:3]
    new_jerk = totals[8:11]
    end_vel = vel_base + half_step * new_acc - twelfth * new_jerk
    end_pos = pos_base + half_step * end_vel - twelfth * new_acc
    snap = snap_base - 3.0 * new_acc + 2.0 * h * new_jerk
    crackle = crackle_base - 2.0 * new_acc + h * new_jerk
    for place, value in enumerate((end_pos, end_vel, new_acc, new_jerk)):
        out_ref[:, place, :] = value
    for place, value in enumerate((snap, crackle)):
        der_ref[:, place, :] = value

    @pl.when(chip < far)
    def _():
        finish(send_sem, 8 * chips)

    @pl.when((chip >= far) & ~last)
    def _():
        finish(send_sem, 8 * chips + 8)

    @pl.when(last)
    def _():
        finish(send_sem, 8 * chips + 14)

    @pl.when((side == 1) & (chip > 0))
    def _():
        finish(pass_sem, 16 * chips - 16)

    if far > 1:
        @pl.when(me == 1)
        def _():
            finish(pass_sem, 16 * far - 16)


def write_out(count, corrected, derivatives, out_ref, der_ref):
    for source, target in ((corrected, out_ref), (derivatives, der_ref)):
        live = lax.broadcasted_iota(jnp.int32, source.shape, 2) < count[0]
        target[...] = jnp.where(live, source[...], 0.0)


def build(n):
    def shards(position, velocity, acceleration, old_jerk, masses, levels, active_count, active_slot):
        stars = position.shape[1]
        cap = active_slot.shape[0]
        corrected, derivatives = pl.pallas_call(
            lambda *refs: kernel(n, *refs),
            out_shape=(
                pltpu.VMEM((3, 4, cap), jnp.float32),
                pltpu.VMEM((3, 2, cap), jnp.float32),
            ),
            in_specs=[pl.BlockSpec(memory_space=pltpu.HBM)] * 7,
            out_specs=(pl.BlockSpec(memory_space=pltpu.VMEM),) * 2,
            scratch_shapes=[
                pltpu.VMEM((4, 8, stars), jnp.float32),
                pltpu.VMEM((1, stars), jnp.float32),
                pltpu.VMEM((1, stars), jnp.int32),
                pltpu.VMEM((1, cap), jnp.int32),
                pltpu.VMEM((8 * n, 1, stars), jnp.float32),
                pltpu.VMEM((16, 6 * LANES), jnp.bfloat16),
                pltpu.VMEM((4, 8, stars), jnp.float32),
                pltpu.VMEM((1, stars), jnp.float32),
                pltpu.VMEM((1, stars), jnp.int32),
                pltpu.VMEM((n // 2, 2, 8, stars), jnp.float32),
                pltpu.SemaphoreType.DMA((2,)),
                pltpu.SemaphoreType.DMA,
                pltpu.SemaphoreType.REGULAR,
                pltpu.SemaphoreType.REGULAR,
                pltpu.SemaphoreType.DMA,
                pltpu.SemaphoreType.DMA,
                pltpu.SemaphoreType.DMA((n // 2,)),
            ],
            compiler_params=pltpu.CompilerParams(collective_id=0, has_side_effects=True),
        )(
            position, velocity, acceleration, old_jerk,
            masses[None, :], levels[None, :], active_slot[None, :],
        )
        corrected = pltpu.with_memory_space_constraint(corrected, pltpu.VMEM)
        derivatives = pltpu.with_memory_space_constraint(derivatives, pltpu.VMEM)
        corrected, derivatives = pl.pallas_call(
            write_out,
            out_shape=(
                jax.ShapeDtypeStruct((3, 4, cap), jnp.float32),
                jax.ShapeDtypeStruct((3, 2, cap), jnp.float32),
            ),
            in_specs=[
                pl.BlockSpec(memory_space=pltpu.SMEM),
                pl.BlockSpec(memory_space=pltpu.VMEM),
                pl.BlockSpec(memory_space=pltpu.VMEM),
            ],
            out_specs=(pl.BlockSpec(memory_space=pltpu.VMEM),) * 2,
        )(active_count, corrected, derivatives)
        return corrected.transpose(1, 0, 2), derivatives.transpose(1, 0, 2)

    return shards


def solution(mesh):
    split = P(("members", "stars"))
    wide = P(None, ("members", "stars"))
    deep = P(None, None, ("members", "stars"))
    return jax.shard_map(
        build(mesh.shape["stars"]),
        mesh=mesh,
        in_specs=(wide, wide, wide, wide, split, split, split, split),
        out_specs=(deep, deep),
        check_vma=False,
    )
```

```python
import jax
import jax.numpy as jnp
from jax import lax
from jax.experimental import pallas as pl
from jax.experimental.pallas import tpu as pltpu
from jax.sharding import PartitionSpec as P

SOFTEN = 0.0025
STEP_BASE = 0.5
LANES = 128
HIGHEST = lax.Precision.HIGHEST


def dot(a, b, contract):
    return lax.dot_general(
        a, b, ((contract[:1], contract[1:]), ((), ())),
        precision=HIGHEST, preferred_element_type=jnp.float32,
    )


def power_of_half(level):
    scale = jnp.full(level.shape, STEP_BASE, jnp.float32)
    for bit in range(5):
        scale = jnp.where((level >> bit) & 1 == 1, scale * 0.5 ** (1 << bit), scale)
    return scale


def each(first, last, body):
    def step(k, carry):
        body(k)
        return carry

    lax.fori_loop(first, last, step, 0)


def predict(pos, vel, acc, jerk, level):
    step = power_of_half(level)
    moved_pos = pos + step * (vel + step * (0.5 * acc + step * jerk / 6.0))
    moved_vel = vel + step * (acc + 0.5 * step * jerk)
    return moved_pos, moved_vel, step


def kernel(n, pos_h, vel_h, acc_h, jerk_h, mass_h, level_h, slot_h,
           out_ref, der_ref,
           data8, mass, level, slot, total, collect, far_data, far_mass, far_level, buf,
           in_sem, raw_sem, mate, ready, send_sem, pass_sem, recv_sem):
    data = tuple(data8.at[k, pl.ds(0, 3)] for k in range(4))
    far_data = tuple(far_data.at[k, pl.ds(0, 3)] for k in range(4)) + (far_mass, far_level)
    me = lax.axis_index("stars")
    stars = pos_h.shape[1]
    cap = slot_h.shape[1]
    chips = n // 2
    chip = me // 2
    side = me % 2
    top = chips - 1
    below = jnp.where(chip == top, top, jnp.minimum(chip, 1))
    above = jnp.where(chip == 0, 1, jnp.where(chip == top, chips, top))
    partner = {"stars": me + 1 - 2 * side}
    mesh = pl.DeviceIdType.MESH

    def finish(semaphore, rows):
        same = total.at[pl.ds(0, rows)]
        pltpu.make_async_copy(same, same, semaphore).wait()

    slot_load = pltpu.make_async_copy(slot_h, slot, in_sem.at[1])
    loads = [
        pltpu.make_async_copy(source, target, in_sem.at[0])
        for source, target in zip(
            (pos_h, vel_h, acc_h, jerk_h, mass_h, level_h), (*data, mass, level)
        )
    ]
    barrier = pltpu.get_barrier_semaphore()
    last = (chip == top) & (side == 0)
    entered = below + jnp.minimum(chip, 1) + 1 - side

    @pl.when(last)
    def _():
        pl.semaphore_wait(barrier, entered)
        for device in range(1):
            for source, target in zip(
                (pos_h, vel_h, acc_h, jerk_h, mass_h, level_h), far_data
            ):
                pltpu.make_async_remote_copy(
                    src_ref=source, dst_ref=target, send_sem=send_sem, recv_sem=raw_sem,
                    device_id={"stars": device}, device_id_type=mesh,
                ).start()

    for load in loads:
        load.start()
    slot_load.start()

    def signal(semaphore, device):
        pl.semaphore_signal(
            semaphore, inc=1, device_id={"stars": device}, device_id_type=mesh
        )

    @pl.when(side == 1)
    def _():
        signal(barrier, me - 1)

    @pl.when((side == 1) | (chip == 0))
    def _():
        each(above, chips, lambda p: signal(barrier, 2 * p + 1))
        each(above, chips, lambda p: signal(barrier, 2 * p))

    @pl.when((entered > 0) & ~last)
    def _():
        pl.semaphore_wait(barrier, entered)

    @pl.when(side == 0)
    def _():
        signal(mate, me + 1)

    @pl.when((chip == top) & (side == 1))
    def _():
        each(0, top, lambda p: signal(ready, 2 * p + 1))

    finish(in_sem.at[0], 14)

    pos, vel, acc, jerk = (ref[...] for ref in data)
    moved_pos, moved_vel, step = predict(pos, vel, acc, jerk, level[...])
    own = buf.at[chip, side]
    own[0:3] = moved_pos
    own[3:6] = moved_vel
    own[6:7] = mass[...]
    own[7:8] = step

    far = chips // 2

    def across(other):
        return pltpu.make_async_remote_copy(
            src_ref=own, dst_ref=own,
            send_sem=send_sem, recv_sem=recv_sem.at[chip],
            device_id={"stars": other}, device_id_type=mesh,
        )

    def half(other, part):
        block = buf.at[other, part]
        return pltpu.make_async_remote_copy(
            src_ref=block, dst_ref=block, send_sem=send_sem, recv_sem=recv_sem.at[other],
            device_id=partner, device_id_type=mesh,
        )

    def down(other):
        block = buf.at[other]
        return pltpu.make_async_remote_copy(
            src_ref=block, dst_ref=block,
            send_sem=pass_sem, recv_sem=recv_sem.at[other],
            device_id=partner, device_id_type=mesh,
        )

    @pl.when((chip >= far) & (side == 0) & ~last)
    def _():
        across(0).start()

    each(0, jnp.minimum(below, 1), lambda p: across(2 * p + 1).start())

    @pl.when((chip >= far) & (side == 1))
    def _():
        across(0).start()

    each(1, below, lambda p: across(2 * p + 1).start())
    swap = across(me + 1 - 2 * side)

    @pl.when(side == 1)
    def _():
        pl.semaphore_wait(mate, 1)

    swap.start()

    slot_load.wait()
    pick = (
        lax.broadcasted_iota(jnp.int32, (stars, cap), 0) == slot[...]
    ).astype(jnp.float32)
    moved = dot(own[...], pick, (1, 0))
    start_pos = dot(pos, pick, (1, 0))
    start_vel = dot(vel, pick, (1, 0))
    start_acc = dot(acc, pick, (1, 0))
    start_jerk = dot(jerk, pick, (1, 0))
    part_of = lax.broadcasted_iota(jnp.int32, collect.shape, 1) // LANES
    row_of = lax.broadcasted_iota(jnp.int32, collect.shape, 0)
    collect[...] = (
        part_of + jnp.where(part_of < 3, 0, 5) == row_of
    ).astype(jnp.float32).astype(jnp.bfloat16)
    h = moved[7:8]
    half_step = 0.5 * h
    twelfth = h * h / 12.0
    vel_base = start_vel + half_step * start_acc + twelfth * start_jerk
    pos_base = start_pos + half_step * start_vel + twelfth * start_acc
    snap_base = 3.0 * start_acc + h * start_jerk
    crackle_base = 2.0 * start_acc + h * start_jerk
    spread = (
        lax.broadcasted_iota(jnp.int32, (8, 6 * LANES), 1) // LANES
        == lax.broadcasted_iota(jnp.int32, (8, 6 * LANES), 0)
    ).astype(jnp.float32)
    spread_targets = dot(moved, spread, (0, 0))
    target = [spread_targets[:, c * LANES:(c + 1) * LANES] for c in range(6)]

    def add_block(j, part, sums):
        sums = list(sums)
        for first in range(0, stars, LANES):
            row = [buf[j, part, c:c + 1, first:first + LANES] for c in range(7)]
            d = [row[c] - target[c] for c in range(3)]
            w = [row[c + 3] - target[c + 3] for c in range(3)]
            q = d[0] * d[0] + d[1] * d[1] + d[2] * d[2] + SOFTEN
            u = lax.rsqrt(q)
            u2 = u * u
            weight = row[6] * u * u2
            radial = (d[0] * w[0] + d[1] * w[1] + d[2] * w[2]) * (3.0 * u2)
            for c in range(3):
                sums[c] += weight * d[c]
                sums[c + 3] += weight * (w[c] - radial * d[c])
        return tuple(sums)

    def arrive(k, sums):
        other = jnp.where(chip == 0, k, chips - k - jnp.where(chips - k > chip, 0, 1))
        copy = down(other)
        if k < chips - 1:
            copy.wait_recv()
        else:
            @pl.when(me > 0)
            def _():
                copy.wait_recv()

            @pl.when(me == 0)
            def _():
                half(k, 1).wait_recv()

        @pl.when((side == 1) & ((chip > 0) | (other < far)))
        def _():
            copy.start()

        sums = add_block(other, 1, sums)
        if k == chips - 1:
            @pl.when(me == 0)
            def _():
                finish(raw_sem, 14)
                block = buf.at[k, 0]
                block[0:3], block[3:6], _ = predict(
                    *(ref[...] for ref in far_data[:4]), far_data[5][...]
                )
                block[6:7] = far_data[4][...]

        return add_block(other, 0, sums)

    sums = add_block(chip, side, (jnp.zeros((cap, LANES), jnp.float32),) * 6)

    @pl.when(chip < top)
    def _():
        pl.semaphore_wait(ready, 1)

        @pl.when(side == 1)
        def _():
            signal(ready, me - 1)

        each(below, chip, lambda p: across(2 * p + 1).start())
        each(chip + 1, chips, lambda p: across(2 * p + 1).start())

    swap.wait_recv()
    sums = add_block(chip, 1 - side, sums)
    for k in range(1, chips):
        sums = arrive(k, sums)

    rest = jnp.concatenate(sums, axis=1)
    totals = None
    for _ in range(3):
        part = rest.astype(jnp.bfloat16)
        rest = rest - part.astype(jnp.float32)
        share = lax.dot_general(
            collect[...], part, (((1,), (1,)), ((), ())), preferred_element_type=jnp.float32
        )
        totals = share if totals is None else totals + share
    new_acc = totals[0:3]
    new_jerk = totals[8:11]
    end_vel = vel_base + half_step * new_acc - twelfth * new_jerk
    end_pos = pos_base + half_step * end_vel - twelfth * new_acc
    snap = snap_base - 3.0 * new_acc + 2.0 * h * new_jerk
    crackle = crackle_base - 2.0 * new_acc + h * new_jerk
    for place, value in enumerate((end_pos, end_vel, new_acc, new_jerk)):
        out_ref[:, place, :] = value
    for place, value in enumerate((snap, crackle)):
        der_ref[:, place, :] = value

    @pl.when(chip < far)
    def _():
        finish(send_sem, 8 * chips)

    @pl.when((chip >= far) & ~last)
    def _():
        finish(send_sem, 8 * chips + 8)

    @pl.when(last)
    def _():
        finish(send_sem, 8 * chips + 14)

    @pl.when((side == 1) & (chip > 0))
    def _():
        finish(pass_sem, 16 * chips - 16)

    if far > 1:
        @pl.when(me == 1)
        def _():
            finish(pass_sem, 16 * far - 16)


def write_out(count, corrected, derivatives, out_ref, der_ref):
    for source, target in ((corrected, out_ref), (derivatives, der_ref)):
        live = lax.broadcasted_iota(jnp.int32, source.shape, 2) < count[0]
        target[...] = jnp.where(live, source[...], 0.0)


def build(n):
    def shards(position, velocity, acceleration, old_jerk, masses, levels, active_count, active_slot):
        stars = position.shape[1]
        cap = active_slot.shape[0]
        corrected, derivatives = pl.pallas_call(
            lambda *refs: kernel(n, *refs),
            out_shape=(
                pltpu.VMEM((3, 4, cap), jnp.float32),
                pltpu.VMEM((3, 2, cap), jnp.float32),
            ),
            in_specs=[pl.BlockSpec(memory_space=pltpu.HBM)] * 7,
            out_specs=(pl.BlockSpec(memory_space=pltpu.VMEM),) * 2,
            scratch_shapes=[
                pltpu.VMEM((4, 8, stars), jnp.float32),
                pltpu.VMEM((1, stars), jnp.float32),
                pltpu.VMEM((1, stars), jnp.int32),
                pltpu.VMEM((1, cap), jnp.int32),
                pltpu.VMEM((8 * n, 1, stars), jnp.float32),
                pltpu.VMEM((16, 6 * LANES), jnp.bfloat16),
                pltpu.VMEM((4, 8, stars), jnp.float32),
                pltpu.VMEM((1, stars), jnp.float32),
                pltpu.VMEM((1, stars), jnp.int32),
                pltpu.VMEM((n // 2, 2, 8, stars), jnp.float32),
                pltpu.SemaphoreType.DMA((2,)),
                pltpu.SemaphoreType.DMA,
                pltpu.SemaphoreType.REGULAR,
                pltpu.SemaphoreType.REGULAR,
                pltpu.SemaphoreType.DMA,
                pltpu.SemaphoreType.DMA,
                pltpu.SemaphoreType.DMA((n // 2,)),
            ],
            compiler_params=pltpu.CompilerParams(collective_id=0, has_side_effects=True),
        )(
            position, velocity, acceleration, old_jerk,
            masses[None, :], levels[None, :], active_slot[None, :],
        )
        corrected = pltpu.with_memory_space_constraint(corrected, pltpu.VMEM)
        derivatives = pltpu.with_memory_space_constraint(derivatives, pltpu.VMEM)
        corrected, derivatives = pl.pallas_call(
            write_out,
            out_shape=(
                jax.ShapeDtypeStruct((3, 4, cap), jnp.float32),
                jax.ShapeDtypeStruct((3, 2, cap), jnp.float32),
            ),
            in_specs=[
                pl.BlockSpec(memory_space=pltpu.SMEM),
                pl.BlockSpec(memory_space=pltpu.VMEM),
                pl.BlockSpec(memory_space=pltpu.VMEM),
            ],
            out_specs=(pl.BlockSpec(memory_space=pltpu.VMEM),) * 2,
        )(active_count, corrected, derivatives)
        return corrected.transpose(1, 0, 2), derivatives.transpose(1, 0, 2)

    return shards


def solution(mesh):
    split = P(("members", "stars"))
    wide = P(None, ("members", "stars"))
    deep = P(None, None, ("members", "stars"))
    return jax.shard_map(
        build(mesh.shape["stars"]),
        mesh=mesh,
        in_specs=(wide, wide, wide, wide, split, split, split, split),
        out_specs=(deep, deep),
        check_vma=False,
    )
```

```python
import jax
import jax.numpy as jnp
from jax import lax
from jax.experimental import pallas as pl
from jax.experimental.pallas import tpu as pltpu
from jax.sharding import PartitionSpec as P

SOFTEN = 0.0025
STEP_BASE = 0.5
LANES = 128
HIGHEST = lax.Precision.HIGHEST


def dot(a, b, contract):
    return lax.dot_general(
        a, b, ((contract[:1], contract[1:]), ((), ())),
        precision=HIGHEST, preferred_element_type=jnp.float32,
    )


def power_of_half(level):
    scale = jnp.full(level.shape, STEP_BASE, jnp.float32)
    for bit in range(5):
        scale = jnp.where((level >> bit) & 1 == 1, scale * 0.5 ** (1 << bit), scale)
    return scale


def each(first, last, body):
    def step(k, carry):
        body(k)
        return carry

    lax.fori_loop(first, last, step, 0)


def predict(pos, vel, acc, jerk, level):
    step = power_of_half(level)
    moved_pos = pos + step * (vel + step * (0.5 * acc + step * jerk / 6.0))
    moved_vel = vel + step * (acc + 0.5 * step * jerk)
    return moved_pos, moved_vel, step


def kernel(n, pos_h, vel_h, acc_h, jerk_h, mass_h, level_h, slot_h,
           out_ref, der_ref,
           data8, mass, level, slot, total, collect, far_data, far_mass, far_level, buf,
           in_sem, raw_sem, mate, ready, send_sem, pass_sem, recv_sem):
    data = tuple(data8.at[k, pl.ds(0, 3)] for k in range(4))
    far_data = tuple(far_data.at[k, pl.ds(0, 3)] for k in range(4)) + (far_mass, far_level)
    me = lax.axis_index("stars")
    stars = pos_h.shape[1]
    cap = slot_h.shape[1]
    chips = n // 2
    chip = me // 2
    side = me % 2
    top = chips - 1
    below = jnp.where(chip == top, top, jnp.minimum(chip, 1))
    above = jnp.where(chip == 0, 1, jnp.where(chip == top, chips, top))
    partner = {"stars": me + 1 - 2 * side}
    mesh = pl.DeviceIdType.MESH

    def finish(semaphore, rows):
        same = total.at[pl.ds(0, rows)]
        pltpu.make_async_copy(same, same, semaphore).wait()

    slot_load = pltpu.make_async_copy(slot_h, slot, in_sem.at[1])
    loads = [
        pltpu.make_async_copy(source, target, in_sem.at[0])
        for source, target in zip(
            (pos_h, vel_h, acc_h, jerk_h, mass_h, level_h), (*data, mass, level)
        )
    ]
    barrier = pltpu.get_barrier_semaphore()
    last = (chip == top) & (side == 0)
    entered = below + jnp.minimum(chip, 1) + 1 - side

    @pl.when(last)
    def _():
        pl.semaphore_wait(barrier, entered)
        for device in range(1):
            for source, target in zip(
                (pos_h, vel_h, acc_h, jerk_h, mass_h, level_h), far_data
            ):
                pltpu.make_async_remote_copy(
                    src_ref=source, dst_ref=target, send_sem=send_sem, recv_sem=raw_sem,
                    device_id={"stars": device}, device_id_type=mesh,
                ).start()

    for load in loads:
        load.start()
    slot_load.start()

    def signal(semaphore, device):
        pl.semaphore_signal(
            semaphore, inc=1, device_id={"stars": device}, device_id_type=mesh
        )

    @pl.when(side == 1)
    def _():
        signal(barrier, me - 1)

    @pl.when((side == 1) | (chip == 0))
    def _():
        each(above, chips, lambda p: signal(barrier, 2 * p + 1))
        each(above, chips, lambda p: signal(barrier, 2 * p))

    @pl.when((entered > 0) & ~last)
    def _():
        pl.semaphore_wait(barrier, entered)

    @pl.when(side == 0)
    def _():
        signal(mate, me + 1)

    @pl.when((chip == top) & (side == 1))
    def _():
        each(0, top, lambda p: signal(ready, 2 * p + 1))

    finish(in_sem.at[0], 14)

    pos, vel, acc, jerk = (ref[...] for ref in data)
    moved_pos, moved_vel, step = predict(pos, vel, acc, jerk, level[...])
    own = buf.at[chip, side]
    sent = buf.at[chip, side, pl.ds(0, 7)]
    own[0:3] = moved_pos
    own[3:6] = moved_vel
    own[6:7] = mass[...]
    own[7:8] = step

    far = chips // 2

    def across(other):
        return pltpu.make_async_remote_copy(
            src_ref=sent, dst_ref=sent,
            send_sem=send_sem, recv_sem=recv_sem.at[chip],
            device_id={"stars": other}, device_id_type=mesh,
        )

    def half(other, part):
        block = buf.at[other, part, pl.ds(0, 7)]
        return pltpu.make_async_remote_copy(
            src_ref=block, dst_ref=block, send_sem=send_sem, recv_sem=recv_sem.at[other],
            device_id=partner, device_id_type=mesh,
        )

    def down(other):
        block = buf.at[other, :, pl.ds(0, 7)]
        return pltpu.make_async_remote_copy(
            src_ref=block, dst_ref=block,
            send_sem=pass_sem, recv_sem=recv_sem.at[other],
            device_id=partner, device_id_type=mesh,
        )

    @pl.when((chip >= far) & (side == 0) & ~last)
    def _():
        across(0).start()

    each(0, jnp.minimum(below, 1), lambda p: across(2 * p + 1).start())

    @pl.when((chip >= far) & (side == 1))
    def _():
        across(0).start()

    each(1, below, lambda p: across(2 * p + 1).start())
    swap = across(me + 1 - 2 * side)

    @pl.when(side == 1)
    def _():
        pl.semaphore_wait(mate, 1)

    swap.start()

    slot_load.wait()
    pick = (
        lax.broadcasted_iota(jnp.int32, (stars, cap), 0) == slot[...]
    ).astype(jnp.float32)
    moved = dot(own[...], pick, (1, 0))
    start_pos = dot(pos, pick, (1, 0))
    start_vel = dot(vel, pick, (1, 0))
    start_acc = dot(acc, pick, (1, 0))
    start_jerk = dot(jerk, pick, (1, 0))
    part_of = lax.broadcasted_iota(jnp.int32, collect.shape, 1) // LANES
    row_of = lax.broadcasted_iota(jnp.int32, collect.shape, 0)
    collect[...] = (
        part_of + jnp.where(part_of < 3, 0, 5) == row_of
    ).astype(jnp.float32).astype(jnp.bfloat16)
    h = moved[7:8]
    half_step = 0.5 * h
    twelfth = h * h / 12.0
    vel_base = start_vel + half_step * start_acc + twelfth * start_jerk
    pos_base = start_pos + half_step * start_vel + twelfth * start_acc
    snap_base = 3.0 * start_acc + h * start_jerk
    crackle_base = 2.0 * start_acc + h * start_jerk
    spread = (
        lax.broadcasted_iota(jnp.int32, (8, 6 * LANES), 1) // LANES
        == lax.broadcasted_iota(jnp.int32, (8, 6 * LANES), 0)
    ).astype(jnp.float32)
    spread_targets = dot(moved, spread, (0, 0))
    target = [spread_targets[:, c * LANES:(c + 1) * LANES] for c in range(6)]

    def add_block(j, part, sums):
        sums = list(sums)
        rows = cap // 2
        for side_of in range(2):
            goal = [t[side_of * rows:(side_of + 1) * rows] for t in target]
            mine = sums[6 * side_of:6 * side_of + 6]
            for first in range(0, stars, LANES):
                row = [buf[j, part, c:c + 1, first:first + LANES] for c in range(7)]
                d = [row[c] - goal[c] for c in range(3)]
                w = [row[c + 3] - goal[c + 3] for c in range(3)]
                q = d[0] * d[0] + d[1] * d[1] + d[2] * d[2] + SOFTEN
                u = lax.rsqrt(q)
                u2 = u * u
                weight = row[6] * u * u2
                radial = (d[0] * w[0] + d[1] * w[1] + d[2] * w[2]) * (3.0 * u2)
                for c in range(3):
                    mine[c] += weight * d[c]
                    mine[c + 3] += weight * (w[c] - radial * d[c])
            sums[6 * side_of:6 * side_of + 6] = mine
        return tuple(sums)

    def arrive(k, sums):
        other = jnp.where(chip == 0, k, chips - k - jnp.where(chips - k > chip, 0, 1))
        copy = down(other)
        if k < chips - 1:
            copy.wait_recv()
        else:
            @pl.when(me > 0)
            def _():
                copy.wait_recv()

            @pl.when(me == 0)
            def _():
                half(k, 1).wait_recv()

        @pl.when((side == 1) & ((chip > 0) | (other < far)))
        def _():
            copy.start()

        sums = add_block(other, 1, sums)
        if k == chips - 1:
            @pl.when(me == 0)
            def _():
                finish(raw_sem, 14)
                block = buf.at[k, 0]
                block[0:3], block[3:6], _ = predict(
                    *(ref[...] for ref in far_data[:4]), far_data[5][...]
                )
                block[6:7] = far_data[4][...]

        return add_block(other, 0, sums)

    sums = add_block(chip, side, (jnp.zeros((cap // 2, LANES), jnp.float32),) * 12)

    @pl.when(chip < top)
    def _():
        pl.semaphore_wait(ready, 1)

        @pl.when(side == 1)
        def _():
            signal(ready, me - 1)

        each(below, chip, lambda p: across(2 * p + 1).start())
        each(chip + 1, chips, lambda p: across(2 * p + 1).start())

    swap.wait_recv()
    sums = add_block(chip, 1 - side, sums)
    for k in range(1, chips):
        sums = arrive(k, sums)

    rest = jnp.concatenate(
        [jnp.concatenate([sums[c], sums[c + 6]], axis=0) for c in range(6)], axis=1
    )
    totals = None
    for _ in range(3):
        part = rest.astype(jnp.bfloat16)
        rest = rest - part.astype(jnp.float32)
        share = lax.dot_general(
            collect[...], part, (((1,), (1,)), ((), ())), preferred_element_type=jnp.float32
        )
        totals = share if totals is None else totals + share
    new_acc = totals[0:3]
    new_jerk = totals[8:11]
    end_vel = vel_base + half_step * new_acc - twelfth * new_jerk
    end_pos = pos_base + half_step * end_vel - twelfth * new_acc
    snap = snap_base - 3.0 * new_acc + 2.0 * h * new_jerk
    crackle = crackle_base - 2.0 * new_acc + h * new_jerk
    for place, value in enumerate((end_pos, end_vel, new_acc, new_jerk)):
        out_ref[:, place, :] = value
    for place, value in enumerate((snap, crackle)):
        der_ref[:, place, :] = value

    @pl.when(chip < far)
    def _():
        finish(send_sem, 7 * chips)

    @pl.when((chip >= far) & ~last)
    def _():
        finish(send_sem, 7 * chips + 7)

    @pl.when(last)
    def _():
        finish(send_sem, 7 * chips + 14)

    @pl.when((side == 1) & (chip > 0))
    def _():
        finish(pass_sem, 14 * chips - 14)

    if far > 1:
        @pl.when(me == 1)
        def _():
            finish(pass_sem, 14 * far - 14)


def write_out(count, corrected, derivatives, out_ref, der_ref):
    for source, target in ((corrected, out_ref), (derivatives, der_ref)):
        live = lax.broadcasted_iota(jnp.int32, source.shape, 2) < count[0]
        target[...] = jnp.where(live, source[...], 0.0)


def build(n):
    def shards(position, velocity, acceleration, old_jerk, masses, levels, active_count, active_slot):
        stars = position.shape[1]
        cap = active_slot.shape[0]
        corrected, derivatives = pl.pallas_call(
            lambda *refs: kernel(n, *refs),
            out_shape=(
                pltpu.VMEM((3, 4, cap), jnp.float32),
                pltpu.VMEM((3, 2, cap), jnp.float32),
            ),
            in_specs=[pl.BlockSpec(memory_space=pltpu.HBM)] * 7,
            out_specs=(pl.BlockSpec(memory_space=pltpu.VMEM),) * 2,
            scratch_shapes=[
                pltpu.VMEM((4, 8, stars), jnp.float32),
                pltpu.VMEM((1, stars), jnp.float32),
                pltpu.VMEM((1, stars), jnp.int32),
                pltpu.VMEM((1, cap), jnp.int32),
                pltpu.VMEM((8 * n, 1, stars), jnp.float32),
                pltpu.VMEM((16, 6 * LANES), jnp.bfloat16),
                pltpu.VMEM((4, 8, stars), jnp.float32),
                pltpu.VMEM((1, stars), jnp.float32),
                pltpu.VMEM((1, stars), jnp.int32),
                pltpu.VMEM((n // 2, 2, 8, stars), jnp.float32),
                pltpu.SemaphoreType.DMA((2,)),
                pltpu.SemaphoreType.DMA,
                pltpu.SemaphoreType.REGULAR,
                pltpu.SemaphoreType.REGULAR,
                pltpu.SemaphoreType.DMA,
                pltpu.SemaphoreType.DMA,
                pltpu.SemaphoreType.DMA((n // 2,)),
            ],
            compiler_params=pltpu.CompilerParams(collective_id=0, has_side_effects=True),
        )(
            position, velocity, acceleration, old_jerk,
            masses[None, :], levels[None, :], active_slot[None, :],
        )
        corrected = pltpu.with_memory_space_constraint(corrected, pltpu.VMEM)
        derivatives = pltpu.with_memory_space_constraint(derivatives, pltpu.VMEM)
        corrected, derivatives = pl.pallas_call(
            write_out,
            out_shape=(
                jax.ShapeDtypeStruct((3, 4, cap), jnp.float32),
                jax.ShapeDtypeStruct((3, 2, cap), jnp.float32),
            ),
            in_specs=[
                pl.BlockSpec(memory_space=pltpu.SMEM),
                pl.BlockSpec(memory_space=pltpu.VMEM),
                pl.BlockSpec(memory_space=pltpu.VMEM),
            ],
            out_specs=(pl.BlockSpec(memory_space=pltpu.VMEM),) * 2,
        )(active_count, corrected, derivatives)
        return corrected.transpose(1, 0, 2), derivatives.transpose(1, 0, 2)

    return shards


def solution(mesh):
    split = P(("members", "stars"))
    wide = P(None, ("members", "stars"))
    deep = P(None, None, ("members", "stars"))
    return jax.shard_map(
        build(mesh.shape["stars"]),
        mesh=mesh,
        in_specs=(wide, wide, wide, wide, split, split, split, split),
        out_specs=(deep, deep),
        check_vma=False,
    )
```

```python
import jax
import jax.numpy as jnp
from jax import lax
from jax.experimental import pallas as pl
from jax.experimental.pallas import tpu as pltpu
from jax.sharding import PartitionSpec as P

SOFTEN = 0.0025
STEP_BASE = 0.5
LANES = 128
HIGHEST = lax.Precision.HIGHEST


def dot(a, b, contract):
    return lax.dot_general(
        a, b, ((contract[:1], contract[1:]), ((), ())),
        precision=HIGHEST, preferred_element_type=jnp.float32,
    )


def power_of_half(level):
    scale = jnp.full(level.shape, STEP_BASE, jnp.float32)
    for bit in range(5):
        scale = jnp.where((level >> bit) & 1 == 1, scale * 0.5 ** (1 << bit), scale)
    return scale


def each(first, last, body):
    def step(k, carry):
        body(k)
        return carry

    lax.fori_loop(first, last, step, 0)


def predict(pos, vel, acc, jerk, level):
    step = power_of_half(level)
    moved_pos = pos + step * (vel + step * (0.5 * acc + step * jerk / 6.0))
    moved_vel = vel + step * (acc + 0.5 * step * jerk)
    return moved_pos, moved_vel, step


def kernel(n, pos_h, vel_h, acc_h, jerk_h, mass_h, level_h, slot_h,
           out_ref, der_ref,
           data8, mass, level, slot, total, collect, far_data, far_mass, far_level, buf,
           in_sem, raw_sem, mate, ready, send_sem, recv_sem):
    data = tuple(data8.at[k, pl.ds(0, 3)] for k in range(4))
    far_data = tuple(far_data.at[k, pl.ds(0, 3)] for k in range(4)) + (far_mass, far_level)
    me = lax.axis_index("stars")
    stars = pos_h.shape[1]
    cap = slot_h.shape[1]
    chips = n // 2
    chip = me // 2
    side = me % 2
    top = chips - 1
    below = jnp.where(chip == top, top, jnp.minimum(chip, 1))
    above = jnp.where(chip == 0, 1, jnp.where(chip == top, chips, top))
    partner = {"stars": me + 1 - 2 * side}
    mesh = pl.DeviceIdType.MESH

    def finish(semaphore, rows):
        same = total.at[pl.ds(0, rows)]
        pltpu.make_async_copy(same, same, semaphore).wait()

    slot_load = pltpu.make_async_copy(slot_h, slot, in_sem.at[1])
    loads = [
        pltpu.make_async_copy(source, target, in_sem.at[0])
        for source, target in zip(
            (pos_h, vel_h, acc_h, jerk_h, mass_h, level_h), (*data, mass, level)
        )
    ]
    barrier = pltpu.get_barrier_semaphore()
    last = (chip == top) & (side == 0)
    entered = below + jnp.minimum(chip, 1) + 1 - side

    @pl.when(last)
    def _():
        pl.semaphore_wait(barrier, entered)
        for device in range(1):
            for source, target in zip(
                (pos_h, vel_h, acc_h, jerk_h, mass_h, level_h), far_data
            ):
                pltpu.make_async_remote_copy(
                    src_ref=source, dst_ref=target, send_sem=send_sem, recv_sem=raw_sem,
                    device_id={"stars": device}, device_id_type=mesh,
                ).start()

    for load in loads:
        load.start()
    slot_load.start()

    def signal(semaphore, device):
        pl.semaphore_signal(
            semaphore, inc=1, device_id={"stars": device}, device_id_type=mesh
        )

    @pl.when(side == 1)
    def _():
        signal(barrier, me - 1)

    @pl.when((side == 1) | (chip == 0))
    def _():
        each(above, chips, lambda p: signal(barrier, 2 * p + 1))
        each(above, chips, lambda p: signal(barrier, 2 * p))

    @pl.when((entered > 0) & ~last)
    def _():
        pl.semaphore_wait(barrier, entered)

    @pl.when(side == 0)
    def _():
        signal(mate, me + 1)

    @pl.when((chip == top) & (side == 1))
    def _():
        each(0, top, lambda p: signal(ready, 2 * p + 1))

    finish(in_sem.at[0], 14)

    pos, vel, acc, jerk = (ref[...] for ref in data)
    moved_pos, moved_vel, step = predict(pos, vel, acc, jerk, level[...])
    own = buf.at[chip, side]
    sent = buf.at[chip, side, pl.ds(0, 7)]
    own[0:3] = moved_pos
    own[3:6] = moved_vel
    own[6:7] = mass[...]
    own[7:8] = step

    far = chips // 2

    def across(other):
        return pltpu.make_async_remote_copy(
            src_ref=sent, dst_ref=sent,
            send_sem=send_sem, recv_sem=recv_sem.at[chip],
            device_id={"stars": other}, device_id_type=mesh,
        )

    def half(other, part):
        block = buf.at[other, part, pl.ds(0, 7)]
        return pltpu.make_async_remote_copy(
            src_ref=block, dst_ref=block, send_sem=send_sem, recv_sem=recv_sem.at[other],
            device_id=partner, device_id_type=mesh,
        )

    def down(other):
        block = buf.at[other, :, pl.ds(0, 7)]
        return pltpu.make_async_remote_copy(
            src_ref=block, dst_ref=block,
            send_sem=send_sem, recv_sem=recv_sem.at[other],
            device_id=partner, device_id_type=mesh,
        )

    @pl.when((chip >= far) & (side == 0) & ~last)
    def _():
        across(0).start()

    each(0, jnp.minimum(below, 1), lambda p: across(2 * p + 1).start())

    @pl.when((chip >= far) & (side == 1))
    def _():
        across(0).start()

    each(1, below, lambda p: across(2 * p + 1).start())
    swap = across(me + 1 - 2 * side)

    @pl.when(side == 1)
    def _():
        pl.semaphore_wait(mate, 1)

    swap.start()

    slot_load.wait()
    pick = (
        lax.broadcasted_iota(jnp.int32, (stars, cap), 0) == slot[...]
    ).astype(jnp.float32)
    moved = dot(own[...], pick, (1, 0))
    start_pos = dot(pos, pick, (1, 0))
    start_vel = dot(vel, pick, (1, 0))
    start_acc = dot(acc, pick, (1, 0))
    start_jerk = dot(jerk, pick, (1, 0))
    part_of = lax.broadcasted_iota(jnp.int32, collect.shape, 1) // LANES
    row_of = lax.broadcasted_iota(jnp.int32, collect.shape, 0)
    collect[...] = (
        part_of + jnp.where(part_of < 3, 0, 5) == row_of
    ).astype(jnp.float32).astype(jnp.bfloat16)
    h = moved[7:8]
    half_step = 0.5 * h
    twelfth = h * h / 12.0
    vel_base = start_vel + half_step * start_acc + twelfth * start_jerk
    pos_base = start_pos + half_step * start_vel + twelfth * start_acc
    snap_base = 3.0 * start_acc + h * start_jerk
    crackle_base = 2.0 * start_acc + h * start_jerk
    spread = (
        lax.broadcasted_iota(jnp.int32, (8, 6 * LANES), 1) // LANES
        == lax.broadcasted_iota(jnp.int32, (8, 6 * LANES), 0)
    ).astype(jnp.float32)
    spread_targets = dot(moved, spread, (0, 0))
    target = [spread_targets[:, c * LANES:(c + 1) * LANES] for c in range(6)]

    def add_block(j, part, sums):
        sums = list(sums)
        rows = cap // 2
        for side_of in range(2):
            goal = [t[side_of * rows:(side_of + 1) * rows] for t in target]
            mine = sums[6 * side_of:6 * side_of + 6]
            for first in range(0, stars, LANES):
                row = [buf[j, part, c:c + 1, first:first + LANES] for c in range(7)]
                d = [row[c] - goal[c] for c in range(3)]
                w = [row[c + 3] - goal[c + 3] for c in range(3)]
                q = d[0] * d[0] + d[1] * d[1] + d[2] * d[2] + SOFTEN
                u = lax.rsqrt(q)
                u2 = u * u
                weight = row[6] * u * u2
                radial = (d[0] * w[0] + d[1] * w[1] + d[2] * w[2]) * (3.0 * u2)
                for c in range(3):
                    mine[c] += weight * d[c]
                    mine[c + 3] += weight * (w[c] - radial * d[c])
            sums[6 * side_of:6 * side_of + 6] = mine
        return tuple(sums)

    def arrive(k, sums):
        other = jnp.where(chip == 0, k, chips - k - jnp.where(chips - k > chip, 0, 1))
        copy = down(other)
        if k < chips - 1:
            copy.wait_recv()
        else:
            @pl.when(me > 0)
            def _():
                copy.wait_recv()

            @pl.when(me == 0)
            def _():
                half(k, 1).wait_recv()

        @pl.when((side == 1) & ((chip > 0) | (other < far)))
        def _():
            copy.start()

        sums = add_block(other, 1, sums)
        if k == chips - 1:
            @pl.when(me == 0)
            def _():
                finish(raw_sem, 14)
                block = buf.at[k, 0]
                block[0:3], block[3:6], _ = predict(
                    *(ref[...] for ref in far_data[:4]), far_data[5][...]
                )
                block[6:7] = far_data[4][...]

        return add_block(other, 0, sums)

    sums = add_block(chip, side, (jnp.zeros((cap // 2, LANES), jnp.float32),) * 12)

    @pl.when(chip < top)
    def _():
        pl.semaphore_wait(ready, 1)

        @pl.when(side == 1)
        def _():
            signal(ready, me - 1)

        each(below, chip, lambda p: across(2 * p + 1).start())
        each(chip + 1, chips, lambda p: across(2 * p + 1).start())

    swap.wait_recv()
    sums = add_block(chip, 1 - side, sums)
    for k in range(1, chips):
        sums = arrive(k, sums)

    rest = jnp.concatenate(
        [jnp.concatenate([sums[c], sums[c + 6]], axis=0) for c in range(6)], axis=1
    )
    totals = None
    for _ in range(3):
        part = rest.astype(jnp.bfloat16)
        rest = rest - part.astype(jnp.float32)
        share = lax.dot_general(
            collect[...], part, (((1,), (1,)), ((), ())), preferred_element_type=jnp.float32
        )
        totals = share if totals is None else totals + share
    new_acc = totals[0:3]
    new_jerk = totals[8:11]
    end_vel = vel_base + half_step * new_acc - twelfth * new_jerk
    end_pos = pos_base + half_step * end_vel - twelfth * new_acc
    snap = snap_base - 3.0 * new_acc + 2.0 * h * new_jerk
    crackle = crackle_base - 2.0 * new_acc + h * new_jerk
    for place, value in enumerate((end_pos, end_vel, new_acc, new_jerk)):
        out_ref[:, place, :] = value
    for place, value in enumerate((snap, crackle)):
        der_ref[:, place, :] = value

    passed = 14 * chips - 14
    for case, rows in (
        ((side == 0) & (chip < far), 7 * chips),
        ((side == 0) & (chip >= far) & ~last, 7 * chips + 7),
        (last, 7 * chips + 14),
        (me == 1, 7 * chips + 14 * far - 14),
        ((side == 1) & (chip > 0) & (chip < far), 7 * chips + passed),
        ((side == 1) & (chip >= far), 7 * chips + 7 + passed),
    ):
        @pl.when(case)
        def _():
            finish(send_sem, rows)


def write_out(count, corrected, derivatives, out_ref, der_ref):
    for source, target in ((corrected, out_ref), (derivatives, der_ref)):
        live = lax.broadcasted_iota(jnp.int32, source.shape, 2) < count[0]
        target[...] = jnp.where(live, source[...], 0.0)


def build(n):
    def shards(position, velocity, acceleration, old_jerk, masses, levels, active_count, active_slot):
        stars = position.shape[1]
        cap = active_slot.shape[0]
        corrected, derivatives = pl.pallas_call(
            lambda *refs: kernel(n, *refs),
            out_shape=(
                pltpu.VMEM((3, 4, cap), jnp.float32),
                pltpu.VMEM((3, 2, cap), jnp.float32),
            ),
            in_specs=[pl.BlockSpec(memory_space=pltpu.HBM)] * 7,
            out_specs=(pl.BlockSpec(memory_space=pltpu.VMEM),) * 2,
            scratch_shapes=[
                pltpu.VMEM((4, 8, stars), jnp.float32),
                pltpu.VMEM((1, stars), jnp.float32),
                pltpu.VMEM((1, stars), jnp.int32),
                pltpu.VMEM((1, cap), jnp.int32),
                pltpu.VMEM((11 * n, 1, stars), jnp.float32),
                pltpu.VMEM((16, 6 * LANES), jnp.bfloat16),
                pltpu.VMEM((4, 8, stars), jnp.float32),
                pltpu.VMEM((1, stars), jnp.float32),
                pltpu.VMEM((1, stars), jnp.int32),
                pltpu.VMEM((n // 2, 2, 8, stars), jnp.float32),
                pltpu.SemaphoreType.DMA((2,)),
                pltpu.SemaphoreType.DMA,
                pltpu.SemaphoreType.REGULAR,
                pltpu.SemaphoreType.REGULAR,
                pltpu.SemaphoreType.DMA,
                pltpu.SemaphoreType.DMA((n // 2,)),
            ],
            compiler_params=pltpu.CompilerParams(collective_id=0, has_side_effects=True),
        )(
            position, velocity, acceleration, old_jerk,
            masses[None, :], levels[None, :], active_slot[None, :],
        )
        corrected = pltpu.with_memory_space_constraint(corrected, pltpu.VMEM)
        derivatives = pltpu.with_memory_space_constraint(derivatives, pltpu.VMEM)
        corrected, derivatives = pl.pallas_call(
            write_out,
            out_shape=(
                jax.ShapeDtypeStruct((3, 4, cap), jnp.float32),
                jax.ShapeDtypeStruct((3, 2, cap), jnp.float32),
            ),
            in_specs=[
                pl.BlockSpec(memory_space=pltpu.SMEM),
                pl.BlockSpec(memory_space=pltpu.VMEM),
                pl.BlockSpec(memory_space=pltpu.VMEM),
            ],
            out_specs=(pl.BlockSpec(memory_space=pltpu.VMEM),) * 2,
        )(active_count, corrected, derivatives)
        return corrected.transpose(1, 0, 2), derivatives.transpose(1, 0, 2)

    return shards


def solution(mesh):
    split = P(("members", "stars"))
    wide = P(None, ("members", "stars"))
    deep = P(None, None, ("members", "stars"))
    return jax.shard_map(
        build(mesh.shape["stars"]),
        mesh=mesh,
        in_specs=(wide, wide, wide, wide, split, split, split, split),
        out_specs=(deep, deep),
        check_vma=False,
    )
```
